256 devices in a mesh: expert: 32 (over x, y, core), dp: 8 (over z).
Axes of the slice: x: 4, y: 4, z: 8, core: 2. Of those that a mesh axis runs over, the one named last changes fastest.
Arguments:
- patches: bfloat16 [65536, 1024], P(('expert', 'dp')), may hold values from -6 to 6
- router_weight: bfloat16 [1024, 32], replicated, may hold values from -0.1875 to 0.1875
- router_bias: float32 [32], replicated, may hold values from -1.5 to 1.5
- noise: float32 [65536, 32], P(('expert', 'dp')), may hold values from -5 to 5
- top_experts: int32 [65536, 2], P(('expert', 'dp')), may hold values from 0 to 31, all different within a row; in each aligned block of 256 rows (0 to 255, 256 to 511, ...) at most 20 rows name the same one
- threshold_expert: int32 [65536], P(('expert', 'dp')), may hold values from 0 to 31
- w_in: bfloat16 [32, 1024, 2048], P('expert'), may hold values from -0.1875 to 0.1875
- w_out: bfloat16 [32, 2048, 1024], P('expert'), may hold values from -0.125 to 0.125
- out_grad: bfloat16 [65536, 1024], P(('expert', 'dp')), may hold values from -24 to 24
Outputs:
- patch_grad: bfloat16 [65536, 1024], P(('expert', 'dp'))
- w_in_grad: bfloat16 [32, 1024, 2048], P('expert', None, 'dp')
- w_out_grad: bfloat16 [32, 2048, 1024], P('expert', 'dp')
- router_weight_grad: float32 [1024, 32], replicated
- router_bias_grad: float32 [32], replicated
The draws below stay inside these ranges and needn't reach their ends.
Inputs may be any that keep to these rules, and one draw needn't show every extreme that they name: `top_experts`: the two experts of a patch differ; among the patches of one device no expert is named more than 20 times.
All inputs are finite; a program needn't handle non-finite values.
Results may differ from the reference program's by a relative error of at most 0.0062.
The reference program's roundings to bfloat16 on the way (of `gates`, `hidden_grad`, `rows_back` and `logit_low`) count: a program that leaves them out, or rounds other values in their place, can miss the bound.
Values may be sent and summed in bfloat16 or wider, within the bound.
A program may use at most 128 MiB of HBM per device.

```python
import math
import jax
import jax.numpy as jnp
import numpy as np
from jax import lax

D = 1024
FFW = 2048
TOK_DEV = 256
E = 32
CAP = 20
TOKENS = 65536


def place_ends(result, own_key, least, largest):
    dims = result.shape
    index_at = [jax.random.randint(jax.random.fold_in(own_key, axis), (), 0, dims[axis]) for axis in range(len(dims))]
    result = result.at[tuple(index_at)].set(least)
    longest = dims.index(max(dims))
    index_at[longest] = (index_at[longest] + 1) % dims[longest]
    return result.at[tuple(index_at)].set(largest)


def level_of(rng, shape, shards, low, high):
    loudness, own = 1.0, jax.random.fold_in(rng, 6)
    for position, shards_of in shards:
        heights = jnp.exp(jax.random.uniform(jax.random.fold_in(own, position), (shards_of,), jnp.float32, low / len(shards), high / len(shards)))
        loudness = loudness * jnp.repeat(heights, shape[position] // shards_of).reshape([-1 if axis == position else 1 for axis in range(len(shape))])
    return loudness


def shared_out(key, own, number, rows, count, top, most, skew):
    order = jax.random.permutation(key, count)
    heavy_load, common = load_shares(count, rows * top, most, skew, True), load_shares(count, rows * top, most, skew, False)
    places = jnp.arange(count)

    def named(sizes, offset_by):
        used = int((sizes > 0).sum())
        fixed = max(1, used // 4)
        moved = fixed + (places - fixed + offset_by * (used - fixed)) % max(1, count - fixed)
        return jnp.zeros((count,), jnp.int32).at[order[jnp.where(places < fixed, places, moved)]].set(jnp.asarray(sizes, jnp.int32))

    sizes = jnp.where(number % 4 == 0, named(heavy_load, number // 4), named(common, number - number // 4 - 1))
    mixed = jax.random.permutation(jax.random.fold_in(own, 3), count)
    donor, taker = mixed[0:count // 2 * 2:2], mixed[1:count // 2 * 2:2]
    slack = jnp.minimum(sizes[donor] - 1, most - sizes[taker]) // 2
    slack = jnp.where((donor == order[0]) | (taker == order[0]) | (sizes[taker] == 0), 0, jnp.maximum(slack, 0))
    moved = jax.random.randint(jax.random.fold_in(own, 4), (count // 2,), 0, 1 << 20) % (slack + 1)
    sizes = sizes.at[donor].add(-moved).at[taker].add(moved)
    members = jnp.searchsorted(jnp.cumsum(sizes), jnp.arange(rows * top), side="right").astype(jnp.int32)
    table = members.reshape(top, rows).T
    table = table[jax.random.permutation(jax.random.fold_in(own, 1), rows)]
    offset_by = jax.random.randint(jax.random.fold_in(own, 2), (rows, 1), 0, top)
    return jnp.take_along_axis(table, (jnp.arange(top)[None, :] + offset_by) % top, axis=1)


def load_shares(count, total, bound, skew, full):
    portions = [(1 << 20) // math.isqrt(grade ** skew) + 1 for grade in range(1, count + 1)]
    largest = bound if full else min(bound, max(-(-total // count), total * portions[0] // sum(portions)))
    least = 1 if total - largest >= count - 1 else 0
    counts, rest = [largest] + [least] * (count - 1), total - largest - least * (count - 1)
    while rest > 0:
        candidates = [i for i in range(1, count) if counts[i] < largest] or [i for i in range(1, count) if counts[i] < bound]
        mass, left = sum([portions[i] for i in candidates]), rest
        for i in candidates:
            addition = min(bound - counts[i], max(1, left * portions[i] // mass), rest)
            counts[i] = counts[i] + addition
            rest = rest - addition
    return np.array(counts)


def scatter_about(key, shape, deviation, limit, pieces=(), kind=jnp.bfloat16):
    drawn = deviation * jax.random.normal(key, shape, jnp.float32)
    if pieces:
        drawn = drawn * level_of(key, shape, pieces, -0.22, 0.18)
    return jnp.clip(drawn, -limit, limit).astype(kind)


def setup_inputs(seed: int = 0) -> dict:
    key_of = jax.random.split(jax.random.key(seed), 10)
    patches = scatter_about(key_of[0], (TOKENS, D), 1.0, 6.0, ((0, 256),))
    router_weight = scatter_about(key_of[1], (D, E), D ** -0.5, 0.1875)
    router_bias = jnp.clip(jax.random.uniform(key_of[2], (E,), jnp.float32, -1.5, 1.5), -1.5, 1.5)
    noise = scatter_about(key_of[3], (TOKENS, E), 1.0, 5.0, ((0, 256),), jnp.float32)
    top_experts_keys = jax.random.split(jax.random.fold_in(key_of[4], 1), TOKENS // TOK_DEV)
    top_experts_turns = jax.random.permutation(jax.random.fold_in(key_of[4], 3), TOKENS // TOK_DEV)
    top_experts = jax.vmap(lambda own, number: shared_out(jax.random.fold_in(key_of[4], 2), own, number, TOK_DEV, E, 2, CAP, 1))(top_experts_keys, top_experts_turns).reshape((TOKENS, 2))
    threshold_expert = place_ends(jax.random.randint(key_of[5], (TOKENS,), 0, E), jax.random.fold_in(key_of[5], 1), 0, E - 1).astype(jnp.int32)
    w_in = scatter_about(key_of[6], (E, D, FFW), D ** -0.5, 0.1875, ((0, 32),))
    w_out = scatter_about(key_of[7], (E, FFW, D), FFW ** -0.5, 0.125, ((0, 32),))
    out_grad = scatter_about(key_of[8], (TOKENS, D), 4.0, 24.0, ((0, 256),))
    return dict(patches=patches, router_weight=router_weight, router_bias=router_bias, noise=noise, top_experts=top_experts, threshold_expert=threshold_expert, w_in=w_in, w_out=w_out, out_grad=out_grad)


noise_std = 1.0
aux_weight = 1.0
inv_root_two = 0.7071067811865476
inv_root_tau = 0.3989422804014327

def gelu_tanh(values):
    return jax.nn.gelu(values, approximate=True)

def spread_grad(values):
    number = values.shape[0]
    average = jnp.mean(values)
    spread = jnp.mean((values - average) ** 2)
    return (2.0 * (values - average) - 2.0 * spread / average) / (number * average * average)

def expert_terms(rows_in, rows_grad, rows_gate, w_first, w_second):
    hidden = jnp.dot(rows_in, w_first, preferred_element_type=jnp.float32)
    active, pullback = jax.vjp(gelu_tanh, hidden)
    active_low = lax.optimization_barrier(active.astype(jnp.bfloat16))
    back_proj = jnp.dot(rows_grad, w_second.T, preferred_element_type=jnp.float32)
    gate_col = rows_gate.astype(jnp.float32)[:, None]
    gate_terms = lax.optimization_barrier(jnp.sum(back_proj * active_low.astype(jnp.float32), axis=-1))
    hidden_grad = pullback(gate_col * back_proj)[0].astype(jnp.bfloat16)
    scaled_grad = (gate_col * rows_grad.astype(jnp.float32)).astype(jnp.bfloat16)
    first_grad = jnp.dot(rows_in.T, hidden_grad, preferred_element_type=jnp.float32)
    second_grad = jnp.dot(active_low.T, scaled_grad, preferred_element_type=jnp.float32)
    rows_back = jnp.dot(hidden_grad, w_first.T, preferred_element_type=jnp.float32)
    return (first_grad, second_grad, rows_back, gate_terms)

def reference(patches, router_weight, router_bias, noise, top_experts, threshold_expert, w_in, w_out, out_grad):
    tokens = patches.shape[0]
    width = patches.shape[1]
    experts = router_weight.shape[1]
    blocks = tokens // TOK_DEV
    logits = jnp.dot(patches, router_weight, preferred_element_type=jnp.float32) + router_bias
    noisy = logits + noise_std * noise
    probs = jax.nn.softmax(noisy, axis=-1)
    expert_ids = lax.broadcasted_iota(jnp.int32, (1, experts), 1)
    thresh_hot = threshold_expert[:, None] == expert_ids
    base = lax.optimization_barrier(jnp.sum(jnp.where(thresh_hot, noisy, 0.0), axis=-1, keepdims=True))
    zscore = (logits - base) / noise_std
    importance = lax.optimization_barrier(jnp.sum(probs, axis=0))
    load = lax.optimization_barrier(jnp.sum(0.5 * (1.0 + lax.erf(zscore * inv_root_two)), axis=0))
    top_hot = top_experts[:, :, None] == expert_ids[None]
    gates = lax.optimization_barrier(jnp.sum(jnp.where(top_hot, probs[:, None, :], 0.0), axis=-1)).astype(jnp.bfloat16)
    flat = top_experts.reshape(blocks, 2 * TOK_DEV)
    flat_hot = (flat[:, :, None] == expert_ids[None]).astype(jnp.int32)
    before = lax.optimization_barrier(jnp.sum((jnp.cumsum(flat_hot, axis=1) - flat_hot) * flat_hot, axis=-1)).astype(jnp.int32)
    slot_rows = (jnp.arange(blocks, dtype=jnp.int32)[:, None] * CAP + before).astype(jnp.int32)
    token_ids = (jnp.arange(2 * tokens, dtype=jnp.int32) // 2).reshape(blocks, 2 * TOK_DEV)
    table = jnp.full((experts, blocks * CAP), tokens, jnp.int32).at[flat, slot_rows].set(token_ids)
    gate_table = jnp.zeros((experts, blocks * CAP), jnp.bfloat16).at[flat, slot_rows].set(gates.reshape(blocks, 2 * TOK_DEV))

    def one_expert(operands):
        w_first, w_second, index_row, gate_row = operands
        valid = (index_row < tokens)[:, None]
        safe = jnp.minimum(index_row, tokens - 1)
        rows_in = jnp.where(valid, patches[safe], jnp.zeros((), jnp.bfloat16))
        rows_grad = jnp.where(valid, out_grad[safe], jnp.zeros((), jnp.bfloat16))
        first_grad, second_grad, rows_back, gate_terms = expert_terms(rows_in, rows_grad, gate_row, w_first, w_second)
        return (first_grad.astype(jnp.bfloat16), second_grad.astype(jnp.bfloat16), rows_back.astype(jnp.bfloat16), gate_terms.astype(jnp.bfloat16))
    first_all, second_all, back_all, gate_all = lax.map(one_expert, (w_in, w_out, table, gate_table))
    picked = back_all[flat, slot_rows].astype(jnp.float32).reshape(tokens, 2, width)
    expert_back = lax.optimization_barrier(jnp.sum(picked, axis=1))
    gate_grad = gate_all[flat, slot_rows].astype(jnp.float32).reshape(tokens, 2)
    total_weight = aux_weight * tokens
    imp_coef = total_weight * spread_grad(importance)
    load_coef = total_weight * spread_grad(load)
    score_grad = lax.optimization_barrier(jnp.sum(jnp.where(top_hot, gate_grad[:, :, None], 0.0), axis=1)) + imp_coef[None, :]
    noisy_grad = probs * (score_grad - lax.optimization_barrier(jnp.sum(probs * score_grad, axis=-1, keepdims=True)))
    z_grad = load_coef[None, :] * inv_root_tau * jnp.exp(-0.5 * zscore * zscore)
    logit_grad = noisy_grad + z_grad / noise_std - jnp.where(thresh_hot, lax.optimization_barrier(jnp.sum(z_grad, axis=-1, keepdims=True)) / noise_std, 0.0)
    logit_low = logit_grad.astype(jnp.bfloat16)
    router_back = jnp.dot(logit_low, router_weight.T, preferred_element_type=jnp.float32)
    patch_grad = (expert_back + router_back).astype(jnp.bfloat16)
    router_weight_grad = jnp.dot(patches.T, logit_low, preferred_element_type=jnp.float32)
    router_bias_grad = lax.optimization_barrier(jnp.sum(logit_grad, axis=0))
    return (patch_grad, first_all, second_all, router_weight_grad, router_bias_grad)
```

```python
import functools
import math

import jax
import jax.numpy as jnp
from jax import lax
from jax.experimental import pallas as pl
from jax.experimental.pallas import tpu as pltpu
from jax.sharding import PartitionSpec as P

F32 = jnp.float32
BF16 = jnp.bfloat16
MESH = pl.DeviceIdType.MESH
MAIN = 16
REST = 4
SPLIT = 4
NSUB = 2
inv_root_two = 0.7071067811865476
inv_root_tau = 0.3989422804014327
gelu_k = math.sqrt(2.0 / math.pi)


def dot(a, b):
    return jnp.dot(a, b, preferred_element_type=F32)


def dot_nt(a, b):
    return lax.dot_general(a, b, (((1,), (1,)), ((), ())), preferred_element_type=F32)


def iota(shape, dim):
    return lax.broadcasted_iota(jnp.int32, shape, dim)


def hot(mask):
    return jnp.where(mask, 1.0, 0.0).astype(BF16)


def wait_bytes(ref, sem):
    pltpu.make_async_copy(ref, ref, sem).wait()


def kernel(
    E, NZ, TOTAL,
    patches, rwT, bias, noiseT, topT, thr, og, w_in_hbm, w_out_hbm,
    pg, wiT, wo, rgT, rb,
    w_in, w_out, w_inT, sel, selr, selT, selrT, send_x, send_g, recv_x, recv_g,
    send_b, recv_b, X, G, SG, AT, HT, rbT, growr, gt, cw0, cw, ccw0, ccw,
    probs_s, z_s, llT_s, stat, sr1, ss2, sr2, ws1, wr1, ws2, wr2, ws3, wr3, wsem, px, ring_sem,
):
    T, D = patches.shape
    F = w_out.shape[0]
    FC = F // NZ
    SUB = FC // NSUB
    QD = D // SPLIT
    S = E * MAIN
    R = E * REST
    ROWS = S + R
    me = lax.axis_index("expert")
    z = lax.axis_index("dp")

    load_in = pltpu.make_async_copy(w_in_hbm, w_in, wsem.at[0])
    load_out = pltpu.make_async_copy(w_out_hbm, w_out, wsem.at[1])
    load_in.start()
    load_out.start()

    barrier = pltpu.get_barrier_semaphore()

    def greet_plane(p, c):
        pl.semaphore_signal(
            barrier, inc=1, device_id=(lax.rem(me + p, E), z), device_id_type=MESH
        )
        return c

    def greet_line(p, c):
        pl.semaphore_signal(
            barrier, inc=1, device_id=(me, lax.rem(z + p, NZ)), device_id_type=MESH
        )
        return c

    lax.fori_loop(1, E, greet_plane, 0)
    lax.fori_loop(1, NZ, greet_line, 0)

    def to_plane(src, by_peer, dst, rows, k):
        def body(i, c):
            half = (i + 1) // 2
            p = half + (1 - lax.rem(i, 2)) * (E - 2 * half)
            peer = lax.rem(me + p, E)
            if by_peer:
                piece = src.at[pl.ds(pl.multiple_of(peer * rows, rows), rows)]
            else:
                piece = src
            pltpu.make_async_remote_copy(
                src_ref=piece,
                dst_ref=dst.at[pl.ds(pl.multiple_of(me * rows, rows), rows)],
                send_sem=px.at[2 * k],
                recv_sem=px.at[2 * k + 1],
                device_id=(peer, z),
                device_id_type=MESH,
            ).start()
            return c

        lax.fori_loop(1, E, body, 0)

    def to_line(src, dst, rows, k):
        def body(p, c):
            pltpu.make_async_remote_copy(
                src_ref=src,
                dst_ref=dst.at[pl.ds(pl.multiple_of(z * rows, rows), rows)],
                send_sem=px.at[2 * k],
                recv_sem=px.at[2 * k + 1],
                device_id=(me, lax.rem(z + p, NZ)),
                device_id_type=MESH,
            ).start()
            return c

        lax.fori_loop(1, NZ, body, 0)

    def own_block(src, by_peer, dst, at, rows):
        here = pl.ds(pl.multiple_of(at * rows, rows), rows)
        dst[here, :] = src[here, :] if by_peer else src[...]

    def received(dst, rows, peers, k):
        wait_bytes(dst.at[pl.ds(0, (peers - 1) * rows)], px.at[2 * k + 1])

    def sent(dst, rows, peers, k):
        wait_bytes(dst.at[pl.ds(0, (peers - 1) * rows)], px.at[2 * k])

    experts = iota((E, T), 0)
    member = (topT[0:1, :] == experts) | (topT[1:2, :] == experts)
    earlier = hot(iota((T, T), 0) < iota((T, T), 1))
    before = dot(hot(member), earlier)
    code = jnp.where(member, before, -1.0).astype(BF16)
    spread = hot(iota((S, E), 0) // MAIN == iota((S, E), 1))
    code_rows = dot(spread, code)
    place = lax.rem(iota((S, T), 0), MAIN)
    sel[...] = hot(code_rows == place.astype(F32))
    is_rest = code_rows == (lax.rem(place, REST) + MAIN).astype(F32)
    for q in range(SPLIT):
        selr[pl.ds(q * S, S), :] = hot(is_rest & (place // REST == q))

    RB = min(S, 128)

    def pack_rows(src, dst):
        def body(i, c):
            rows = pl.ds(pl.multiple_of(i * RB, RB), RB)
            dst[rows, 0:D] = dot(sel[rows, :], src[...]).astype(BF16)
            acc = jnp.zeros((RB, QD), F32)
            for q in range(SPLIT):
                pick = selr[pl.ds(pl.multiple_of(q * S + i * RB, RB), RB), :]
                acc += dot(pick, src[:, q * QD : (q + 1) * QD])
            dst[rows, D : D + QD] = acc.astype(BF16)
            return c

        lax.fori_loop(0, S // RB, body, 0)

    pack_rows(patches, send_x)
    pl.semaphore_wait(barrier, E + NZ - 2)
    to_plane(send_x, True, recv_x, MAIN, 0)
    own_block(send_x, True, recv_x, me, MAIN)

    logits = dot_nt(rwT[...], patches[...]) + bias[...]
    noisy = logits + noiseT[...]
    top = jnp.max(noisy, axis=0, keepdims=True)
    powers = jnp.exp(noisy - top)
    probs = powers / jnp.sum(powers, axis=0, keepdims=True)
    thresh = thr[...] == experts
    base = jnp.sum(jnp.where(thresh, noisy, 0.0), axis=0, keepdims=True)
    zscore = logits - base
    probs_s[...] = probs
    z_s[...] = zscore
    prob_rows = dot(spread, probs.astype(BF16))
    gate_main = jnp.sum(prob_rows * sel[...].astype(F32), axis=1, keepdims=True)
    gate_rest = jnp.sum(jnp.where(is_rest, prob_rows, 0.0), axis=1, keepdims=True)
    low_lanes = iota((S, 128), 1) < 64
    send_g[:, D + QD : D + QD + 128] = jnp.where(low_lanes, gate_main, gate_rest).astype(BF16)
    pack_rows(og, send_g)
    to_plane(send_g, True, recv_g, MAIN, 1)
    own_block(send_g, True, recv_g, me, MAIN)

    importance = jnp.sum(probs, axis=1, keepdims=True)
    load = jnp.sum(0.5 * (1.0 + lax.erf(zscore * inv_root_two)), axis=1, keepdims=True)
    row_id = iota((E, 128), 0)
    lane_id = iota((E, 128), 1)
    both = jnp.where(lane_id == row_id, importance, 0.0) + jnp.where(
        lane_id == row_id + E, load, 0.0
    )
    stat[...] = jnp.broadcast_to(jnp.sum(both, axis=0, keepdims=True), (8, 128))
    to_plane(stat, False, sr1, 8, 2)
    own_block(stat, False, sr1, me, 8)

    eye_t = hot(iota((T, T), 0) == iota((T, T), 1))
    selT[...] = dot_nt(eye_t, sel[...]).astype(BF16)
    for q in range(SPLIT):
        selrT[pl.ds(q * T, T), :] = dot_nt(eye_t, selr[pl.ds(q * S, S), :]).astype(BF16)
    load_in.wait()
    load_out.wait()

    def turn(i, c):
        cols = pl.ds(pl.multiple_of(i * 256, 256), 256)
        w_inT[cols, :] = w_in[:, cols].T
        return c

    lax.fori_loop(0, F // 256, turn, 0)

    def unpack_pick(q):
        r = iota((R, S), 0)
        return hot(iota((R, S), 1) == (r // REST) * MAIN + q * REST + lax.rem(r, REST))

    def pack_pick(q):
        r = iota((S, R), 1)
        return hot(iota((S, R), 0) == (r // REST) * MAIN + q * REST + lax.rem(r, REST))

    def unpack(src, dst):
        dst[0:S, :] = src[:, 0:D]
        for q in range(SPLIT):
            dst[S:ROWS, q * QD : (q + 1) * QD] = dot(
                unpack_pick(q), src[:, D : D + QD]
            ).astype(BF16)

    received(recv_x, MAIN, E, 0)
    unpack(recv_x, X)
    received(recv_g, MAIN, E, 1)
    unpack(recv_g, G)
    gate_tile = recv_g[:, D + QD : D + QD + 128]
    rest_tile = dot(unpack_pick(0), gate_tile)
    gate_col = jnp.concatenate(
        [
            jnp.broadcast_to(gate_tile[:, 0:1].astype(F32), (S, 128)),
            jnp.broadcast_to(rest_tile[:, 64:65], (R, 128)),
        ],
        axis=0,
    )
    SG[...] = (gate_col[:, 0:1] * G[...].astype(F32)).astype(BF16)
    growr[...] = dot_nt(hot(iota((8, 128), 1) == 0), gate_col.astype(BF16))
    gt[...] = jnp.zeros_like(gt)

    def chunk(c):
        rows = pl.ds(pl.multiple_of(c * FC, FC), FC)
        hidden = dot_nt(w_inT[rows, :], X[...])
        back = dot_nt(w_out[rows, :], G[...])
        square = hidden * hidden
        t = jnp.tanh(gelu_k * (hidden + 0.044715 * (square * hidden)))
        cdf = 0.5 * (1.0 + t)
        active = (hidden * cdf).astype(BF16)
        AT[rows, :] = active
        slope = cdf + hidden * (0.5 * (1.0 - t * t)) * (
            gelu_k * (1.0 + (3.0 * 0.044715) * square)
        )
        HT[rows, :] = ((growr[0:1, :] * back) * slope).astype(BF16)
        gt[0:1, :] += jnp.sum(back * active.astype(F32), axis=0, keepdims=True)

    def at_offset(o):
        return lax.rem(z + o + 2 * NZ, NZ)

    def line_copy(src, buf, s, h, to, k):
        i = s * NSUB + h
        return pltpu.make_async_remote_copy(
            src_ref=src,
            dst_ref=buf.at[pl.ds(pl.multiple_of(i * SUB, SUB), SUB)],
            send_sem=ring_sem.at[2 * k, i],
            recv_sem=ring_sem.at[2 * k + 1, i],
            device_id=(me, to),
            device_id_type=MESH,
        )

    ways = ((AT, SG, cw0, cw, -1), (HT, X, ccw0, ccw, 1))

    def ring_step(s):
        def body(h, c):
            for k, (left, right, buf0, buf, sign) in enumerate(ways):
                src_chunk = at_offset(sign * (1 + s))
                rows = pl.ds(pl.multiple_of(src_chunk * FC + h * SUB, SUB), SUB)
                own = dot(left[rows, :], right[...])
                if s == 0:
                    place_at = buf0.at[pl.ds(pl.multiple_of(h * SUB, SUB), SUB)]
                    place_at[...] = own.astype(BF16)
                else:
                    i = (s - 1) * NSUB + h
                    place_at = buf.at[pl.ds(pl.multiple_of(i * SUB, SUB), SUB)]
                    wait_bytes(place_at, ring_sem.at[2 * k + 1, i])
                    place_at[...] = (own + place_at[...].astype(F32)).astype(BF16)
                line_copy(place_at, buf, s, h, at_offset(-sign), k).start()
            return c

        lax.fori_loop(0, NSUB, body, 0)

    def ring_end():
        outs = (wo, wiT)

        def body(h, c):
            for k, (left, right, buf0, buf, sign) in enumerate(ways):
                rows = pl.ds(pl.multiple_of(z * FC + h * SUB, SUB), SUB)
                own = dot(left[rows, :], right[...])
                i = (NZ - 2) * NSUB + h
                last = buf.at[pl.ds(pl.multiple_of(i * SUB, SUB), SUB)]
                wait_bytes(last, ring_sem.at[2 * k + 1, i])
                here = pl.ds(pl.multiple_of(h * SUB, SUB), SUB)
                outs[k][here, :] = (own + last[...].astype(F32)).astype(BF16)
            return c

        lax.fori_loop(0, NSUB, body, 0)

    computed = set()

    def ensure(offsets):
        for o in offsets:
            if o % NZ not in computed:
                computed.add(o % NZ)
                chunk(at_offset(o))

    def pair(s):
        if 2 * (1 + s) < NZ:
            computed.update({(1 + s) % NZ, (-1 - s) % NZ})

            def body(i, c):
                chunk(at_offset((2 * i - 1) * (1 + s)))
                return c

            lax.fori_loop(0, 2, body, 0)
        else:
            ensure((-1 - s, 1 + s))

    def stats_on():
        received(sr1, 8, E, 2)
        total = sr1[0:8, :]
        for j in range(1, E):
            total += sr1[j * 8 : (j + 1) * 8, :]
        ss2[...] = total
        to_line(ss2, sr2, 8, 3)
        own_block(ss2, False, sr2, z, 8)

    def rows_home():
        ensure(range(NZ))

        def body(i, c):
            rows = pl.ds(pl.multiple_of(i * QD, QD), QD)
            rbT[rows, :] = dot(w_in[rows, :], HT[...]).astype(BF16)
            return c

        lax.fori_loop(0, SPLIT, body, 0)
        eye_s = hot(iota((S, S), 0) == iota((S, S), 1))
        rest = jnp.zeros((S, QD), F32)
        for q in range(SPLIT):
            cols = slice(q * QD, (q + 1) * QD)
            send_b[:, cols] = dot_nt(eye_s, rbT[cols, 0:S]).astype(BF16)
            rest += dot_nt(pack_pick(q), rbT[cols, S:ROWS])
        send_b[:, D : D + QD] = rest.astype(BF16)
        terms = jnp.broadcast_to(gt[0:1, :], (128, ROWS)).astype(BF16)
        r = iota((S, R), 1)
        s_ = iota((S, R), 0)
        any_pick = hot((s_ // MAIN == r // REST) & (lax.rem(s_, REST) == lax.rem(r, REST)))
        term_main = dot_nt(eye_s, terms[:, 0:S])
        term_rest = dot_nt(any_pick, terms[:, S:ROWS])
        send_b[:, D + QD : D + QD + 128] = jnp.where(
            iota((S, 128), 1) < 64, term_main, term_rest
        ).astype(BF16)
        to_plane(send_b, True, recv_b, MAIN, 4)
        own_block(send_b, True, recv_b, me, MAIN)

    def spread_grad(v):
        average = jnp.mean(v, axis=0, keepdims=True)
        dev = jnp.mean((v - average) ** 2, axis=0, keepdims=True)
        return (2.0 * (v - average) - 2.0 * dev / average) / (E * average * average)

    def at_home():
        received(sr2, 8, NZ, 3)
        received(recv_b, MAIN, E, 4)
        total = sr2[0:8, :]
        for j in range(1, NZ):
            total += sr2[j * 8 : (j + 1) * 8, :]
        row = jnp.broadcast_to(total[0:1, :], (E, 128))
        imp = jnp.sum(jnp.where(lane_id == row_id, row, 0.0), axis=1, keepdims=True)
        ld = jnp.sum(jnp.where(lane_id == row_id + E, row, 0.0), axis=1, keepdims=True)
        imp_coef = TOTAL * spread_grad(imp)
        load_coef = TOTAL * spread_grad(ld)
        probs = probs_s[...]
        zscore = z_s[...]
        tile = recv_b[:, D + QD : D + QD + 128].astype(F32)
        weighted = sel[...].astype(F32) * tile[:, 0:1] + selr[0:S, :].astype(F32) * tile[:, 64:65]
        gather = hot(iota((E, S), 1) // MAIN == iota((E, S), 0))
        score = dot(gather, weighted.astype(BF16)) + imp_coef
        noisy_grad = probs * (score - jnp.sum(probs * score, axis=0, keepdims=True))
        z_grad = load_coef * inv_root_tau * jnp.exp(-0.5 * zscore * zscore)
        thresh = thr[...] == iota((E, T), 0)
        logit_grad = (
            noisy_grad
            + z_grad
            - jnp.where(thresh, jnp.sum(z_grad, axis=0, keepdims=True), 0.0)
        )
        low = logit_grad.astype(BF16)
        llT_s[...] = low
        weight_part = dot(low, patches[...])
        bias_col = jnp.sum(logit_grad, axis=1, keepdims=True)
        bias_row = jnp.sum(jnp.where(lane_id == row_id, bias_col, 0.0), axis=0, keepdims=True)
        bias_tile = jnp.broadcast_to(bias_row, (8, 128))
        tiles = D // 128
        for p in range(E):
            a, b = p // tiles, p % tiles
            ws1[p * 16 : p * 16 + 8, :] = weight_part[a * 8 : a * 8 + 8, b * 128 : b * 128 + 128]
            ws1[p * 16 + 8 : p * 16 + 16, :] = bias_tile
        to_plane(ws1, True, wr1, 16, 5)
        own_block(ws1, True, wr1, me, 16)
        low_rows = dot_nt(eye_t, llT_s[...]).astype(BF16)
        for q in range(SPLIT):
            cols = slice(q * QD, (q + 1) * QD)
            out = dot(selT[...], recv_b[:, cols])
            out += dot(selrT[pl.ds(q * T, T), :], recv_b[:, D : D + QD])
            out += dot(low_rows, rwT[:, cols])
            pg[:, cols] = out.astype(BF16)

    def reduce_plane():
        received(wr1, 16, E, 5)
        total = wr1[0:16, :]
        for j in range(1, E):
            total += wr1[j * 16 : (j + 1) * 16, :]
        ws2[...] = total
        to_line(ws2, wr2, 16, 6)
        own_block(ws2, False, wr2, z, 16)

    def reduce_line():
        received(wr2, 16, NZ, 6)
        total = wr2[0:16, :]
        for j in range(1, NZ):
            total += wr2[j * 16 : (j + 1) * 16, :]
        rb[...] = total[8:16, :]
        ws3[...] = total[0:8, :]
        to_plane(ws3, False, wr3, 8, 7)
        own_block(ws3, False, wr3, me, 8)

    def spread_total():
        received(wr3, 8, E, 7)
        tiles = D // 128
        for p in range(E):
            a, b = p // tiles, p % tiles
            rgT[a * 8 : a * 8 + 8, b * 128 : b * 128 + 128] = wr3[p * 8 : p * 8 + 8, :]

    hooks = {}
    late = []
    for k, work in enumerate((rows_home, at_home, reduce_plane, reduce_line, spread_total)):
        at = NZ - 5 + k
        if NZ // 2 - 1 <= NZ - 5 and at < NZ - 1:
            hooks[at] = work
        else:
            late.append(work)
    for s in range(NZ - 1):
        pair(s)
        ring_step(s)
        if s == 0:
            stats_on()
        if s in hooks:
            hooks[s]()
    ensure(range(NZ))
    ring_end()
    for work in late:
        work()

    sent(recv_x, MAIN, E, 0)
    sent(recv_g, MAIN, E, 1)
    sent(sr1, 8, E, 2)
    sent(sr2, 8, NZ, 3)
    sent(recv_b, MAIN, E, 4)
    sent(wr1, 16, E, 5)
    sent(wr2, 16, NZ, 6)
    sent(wr3, 8, E, 7)

    def drain(i, c):
        for k, way in enumerate(ways):
            wait_bytes(way[2].at[pl.ds(0, SUB)], ring_sem.at[2 * k, i])
        return c

    lax.fori_loop(0, (NZ - 1) * NSUB, drain, 0)


def on_device(
    patches, router_weight, router_bias, noise, top_experts, threshold_expert, w_in, w_out, out_grad
):
    T, D = patches.shape
    E = router_weight.shape[1]
    NZ = lax.axis_size("dp")
    F = w_in.shape[2]
    FC = F // NZ
    S = E * MAIN
    ROWS = S + E * REST
    QD = D // SPLIT
    WX = D + QD
    WG = WX + 128
    VMEM = pltpu.VMEM
    whole = pl.BlockSpec(memory_space=pltpu.VMEM)
    far = pl.BlockSpec(memory_space=pl.ANY)
    pg, wiT, wo, rgT, rb = pl.pallas_call(
        functools.partial(kernel, E, NZ, float(T * E * NZ)),
        out_shape=(
            jax.ShapeDtypeStruct((T, D), BF16),
            jax.ShapeDtypeStruct((FC, D), BF16),
            jax.ShapeDtypeStruct((FC, D), BF16),
            jax.ShapeDtypeStruct((E, D), F32),
            jax.ShapeDtypeStruct((8, 128), F32),
        ),
        in_specs=[whole] * 7 + [far] * 2,
        out_specs=(whole,) * 5,
        scratch_shapes=[
            VMEM((D, F), BF16), VMEM((F, D), BF16), VMEM((F, D), BF16),
            VMEM((S, T), BF16), VMEM((SPLIT * S, T), BF16),
            VMEM((T, S), BF16), VMEM((SPLIT * T, S), BF16),
            VMEM((S, WX), BF16), VMEM((S, WG), BF16), VMEM((S, WX), BF16), VMEM((S, WG), BF16),
            VMEM((S, WG), BF16), VMEM((S, WG), BF16),
            VMEM((ROWS, D), BF16), VMEM((ROWS, D), BF16), VMEM((ROWS, D), BF16),
            VMEM((F, ROWS), BF16), VMEM((F, ROWS), BF16), VMEM((D, ROWS), BF16),
            VMEM((8, ROWS), F32), VMEM((8, ROWS), F32),
            VMEM((FC, D), BF16), VMEM(((NZ - 1) * FC, D), BF16),
            VMEM((FC, D), BF16), VMEM(((NZ - 1) * FC, D), BF16),
            VMEM((E, T), F32), VMEM((E, T), F32), VMEM((E, T), BF16),
            VMEM((8, 128), F32), VMEM((E * 8, 128), F32),
            VMEM((8, 128), F32), VMEM((NZ * 8, 128), F32),
            VMEM((E * 16, 128), F32), VMEM((E * 16, 128), F32),
            VMEM((16, 128), F32), VMEM((NZ * 16, 128), F32),
            VMEM((8, 128), F32), VMEM((E * 8, 128), F32),
            pltpu.SemaphoreType.DMA((2,)),
            pltpu.SemaphoreType.DMA((16,)),
            pltpu.SemaphoreType.DMA((4, (NZ - 1) * NSUB)),
        ],
        compiler_params=pltpu.CompilerParams(
            collective_id=0, has_side_effects=True, vmem_limit_bytes=63 * 1024 * 1024
        ),
        name="moe_back",
    )(
        patches,
        router_weight.T,
        router_bias.reshape(E, 1),
        noise.T,
        top_experts.T,
        threshold_expert.reshape(1, T),
        out_grad,
        w_in[0],
        w_out[0],
    )
    return (pg, wiT.T[None], wo[None], rgT.T, rb[0, :E])


def solution(mesh):
    both = ("expert", "dp")
    in_specs = (
        P(both, None), P(), P(), P(both, None), P(both, None), P(both),
        P("expert", None, None), P("expert", None, None), P(both, None),
    )
    out_specs = (P(both, None), P("expert", None, "dp"), P("expert", "dp", None), P(), P())
    return jax.shard_map(
        on_device, mesh=mesh, in_specs=in_specs, out_specs=out_specs, check_vma=False
    )
```

```python
import functools
import math

import jax
import jax.numpy as jnp
from jax import lax
from jax.experimental import pallas as pl
from jax.experimental.pallas import tpu as pltpu
from jax.sharding import PartitionSpec as P

F32 = jnp.float32
BF16 = jnp.bfloat16
MESH = pl.DeviceIdType.MESH
MAIN = 16
REST = 4
SPLIT = 4
NSUB = 4
inv_root_two = 0.7071067811865476
inv_root_tau = 0.3989422804014327
gelu_k = math.sqrt(2.0 / math.pi)


def dot(a, b):
    return jnp.dot(a, b, preferred_element_type=F32)


def dot_nt(a, b):
    return lax.dot_general(a, b, (((1,), (1,)), ((), ())), preferred_element_type=F32)


def iota(shape, dim):
    return lax.broadcasted_iota(jnp.int32, shape, dim)


def hot(mask):
    return jnp.where(mask, 1.0, 0.0).astype(BF16)


def wait_bytes(ref, sem):
    pltpu.make_async_copy(ref, ref, sem).wait()


def kernel(
    E, NZ, TOTAL,
    patches_hbm, rwT, bias, noiseT, topT, thr, og_hbm, w_in_hbm, w_out_hbm,
    pg, wiT, wo, rgT, rb,
    patches, og, w_in, w_out, w_inT, picks, slope, own, sel, selr, selT, selrT, send_x, send_g, recv_x, recv_g,
    send_b, recv_b, X, G, SG, AT, HT, rbT, growr, gt, cw0, cw, ccw0, ccw,
    probs_s, z_s, llT_s, stat, sr1, ss2, sr2, ws1, wr1, ws2, wr2, ws3, wr3, wsem, px, ring_sem,
):
    T, D = patches.shape
    F = w_out.shape[0]
    FC = F // NZ
    SUB = FC // NSUB
    QD = D // SPLIT
    S = E * MAIN
    R = E * REST
    ROWS = S + R
    me = lax.axis_index("expert")
    z = lax.axis_index("dp")

    load_patches = pltpu.make_async_copy(patches_hbm, patches, wsem.at[2])
    load_og = pltpu.make_async_copy(og_hbm, og, wsem.at[3])
    load_patches.start()
    load_og.start()
    load_in = pltpu.make_async_copy(w_in_hbm, w_in, wsem.at[0])
    load_out = pltpu.make_async_copy(w_out_hbm, w_out, wsem.at[1])
    load_in.start()
    load_out.start()

    barrier = pltpu.get_barrier_semaphore()

    def greet_plane(p, c):
        pl.semaphore_signal(
            barrier, inc=1, device_id=(lax.rem(me + p, E), z), device_id_type=MESH
        )
        return c

    def greet_line(p, c):
        pl.semaphore_signal(
            barrier, inc=1, device_id=(me, lax.rem(z + p, NZ)), device_id_type=MESH
        )
        return c

    lax.fori_loop(1, E, greet_plane, 0)
    lax.fori_loop(1, NZ, greet_line, 0)

    def to_plane(src, by_peer, dst, rows, k):
        def body(i, c):
            half = (i + 1) // 2
            p = half + (1 - lax.rem(i, 2)) * (E - 2 * half)
            peer = lax.rem(me + p, E)
            if by_peer:
                piece = src.at[pl.ds(pl.multiple_of(peer * rows, rows), rows)]
            else:
                piece = src
            pltpu.make_async_remote_copy(
                src_ref=piece,
                dst_ref=dst.at[pl.ds(pl.multiple_of(me * rows, rows), rows)],
                send_sem=px.at[2 * k],
                recv_sem=px.at[2 * k + 1],
                device_id=(peer, z),
                device_id_type=MESH,
            ).start()
            return c

        lax.fori_loop(1, E, body, 0)

    def to_line(src, dst, rows, k):
        def body(p, c):
            pltpu.make_async_remote_copy(
                src_ref=src,
                dst_ref=dst.at[pl.ds(pl.multiple_of(z * rows, rows), rows)],
                send_sem=px.at[2 * k],
                recv_sem=px.at[2 * k + 1],
                device_id=(me, lax.rem(z + p, NZ)),
                device_id_type=MESH,
            ).start()
            return c

        lax.fori_loop(1, NZ, body, 0)

    def own_block(src, by_peer, dst, at, rows):
        here = pl.ds(pl.multiple_of(at * rows, rows), rows)
        dst[here, :] = src[here, :] if by_peer else src[...]

    def received(dst, rows, peers, k):
        wait_bytes(dst.at[pl.ds(0, (peers - 1) * rows)], px.at[2 * k + 1])

    def sent(dst, rows, peers, k):
        wait_bytes(dst.at[pl.ds(0, (peers - 1) * rows)], px.at[2 * k])

    experts = iota((E, T), 0)
    member = (topT[0:1, :] == experts) | (topT[1:2, :] == experts)
    earlier = hot(iota((T, T), 0) < iota((T, T), 1))
    before = dot(hot(member), earlier)
    code = jnp.where(member, before, -1.0).astype(BF16)
    spread = hot(iota((S, E), 0) // MAIN == iota((S, E), 1))
    code_rows = dot(spread, code)
    place = lax.rem(iota((S, T), 0), MAIN)
    sel[...] = hot(code_rows == place.astype(F32))
    is_rest = code_rows == (lax.rem(place, REST) + MAIN).astype(F32)
    for q in range(SPLIT):
        selr[pl.ds(q * S, S), :] = hot(is_rest & (place // REST == q))

    RB = min(S, 128)

    def pack_rows(src, dst):
        def body(i, c):
            rows = pl.ds(pl.multiple_of(i * RB, RB), RB)
            dst[rows, 0:D] = dot(sel[rows, :], src[...]).astype(BF16)
            acc = jnp.zeros((RB, QD), F32)
            for q in range(SPLIT):
                pick = selr[pl.ds(pl.multiple_of(q * S + i * RB, RB), RB), :]
                acc += dot(pick, src[:, q * QD : (q + 1) * QD])
            dst[rows, D : D + QD] = acc.astype(BF16)
            return c

        lax.fori_loop(0, S // RB, body, 0)

    load_patches.wait()
    pack_rows(patches, send_x)
    pl.semaphore_wait(barrier, E + NZ - 2)
    to_plane(send_x, True, recv_x, MAIN, 0)
    own_block(send_x, True, recv_x, me, MAIN)

    bias_pick = iota((E, E), 0) == iota((E, E), 1)
    bias_rows = jnp.sum(jnp.where(bias_pick, bias[...], 0.0), axis=1, keepdims=True)
    logits = dot_nt(rwT[...], patches[...]) + bias_rows
    noisy = logits + noiseT[...]
    top = jnp.max(noisy, axis=0, keepdims=True)
    powers = jnp.exp(noisy - top)
    probs = powers / jnp.sum(powers, axis=0, keepdims=True)
    thresh = thr[...] == experts
    base = jnp.sum(jnp.where(thresh, noisy, 0.0), axis=0, keepdims=True)
    zscore = logits - base
    probs_s[...] = probs
    z_s[...] = zscore
    prob_rows = dot(spread, probs.astype(BF16))
    gate_main = jnp.sum(prob_rows * sel[...].astype(F32), axis=1, keepdims=True)
    gate_rest = jnp.sum(jnp.where(is_rest, prob_rows, 0.0), axis=1, keepdims=True)
    low_lanes = iota((S, 128), 1) < 64
    send_g[:, D + QD : D + QD + 128] = jnp.where(low_lanes, gate_main, gate_rest).astype(BF16)
    load_og.wait()
    pack_rows(og, send_g)
    to_plane(send_g, True, recv_g, MAIN, 1)
    own_block(send_g, True, recv_g, me, MAIN)

    importance = jnp.sum(probs, axis=1, keepdims=True)
    load = jnp.sum(0.5 * (1.0 + lax.erf(zscore * inv_root_two)), axis=1, keepdims=True)
    row_id = iota((E, 128), 0)
    lane_id = iota((E, 128), 1)
    both = jnp.where(lane_id == row_id, importance, 0.0) + jnp.where(
        lane_id == row_id + E, load, 0.0
    )
    stat[...] = jnp.broadcast_to(jnp.sum(both, axis=0, keepdims=True), (8, 128))
    to_plane(stat, False, sr1, 8, 2)
    own_block(stat, False, sr1, me, 8)

    eye_t = hot(iota((T, T), 0) == iota((T, T), 1))
    selT[...] = dot_nt(eye_t, sel[...]).astype(BF16)
    for q in range(SPLIT):
        selrT[pl.ds(q * T, T), :] = dot_nt(eye_t, selr[pl.ds(q * S, S), :]).astype(BF16)
    for q in range(SPLIT):
        r = iota((R, S), 0)
        picks[pl.ds(q * R, R), :] = hot(
            iota((R, S), 1) == (r // REST) * MAIN + q * REST + lax.rem(r, REST)
        )
    load_in.wait()
    load_out.wait()

    def turn(i, c):
        cols = pl.ds(pl.multiple_of(i * 256, 256), 256)
        w_inT[cols, :] = w_in[:, cols].T
        return c

    lax.fori_loop(0, F // 256, turn, 0)

    def unpack_pick(q):
        return picks[pl.ds(q * R, R), :]

    def pack_pick(q):
        r = iota((S, R), 1)
        return hot(iota((S, R), 0) == (r // REST) * MAIN + q * REST + lax.rem(r, REST))

    def unpack(src, dst):
        dst[0:S, :] = src[:, 0:D]
        for q in range(SPLIT):
            dst[S:ROWS, q * QD : (q + 1) * QD] = dot(
                unpack_pick(q), src[:, D : D + QD]
            ).astype(BF16)

    def chunk_a(c, carry):
        rows = pl.ds(pl.multiple_of(c * FC, FC), FC)
        hidden = dot_nt(w_inT[rows, :], X[...])
        square = hidden * hidden
        t = jnp.tanh(gelu_k * (hidden + 0.044715 * (square * hidden)))
        cdf = 0.5 * (1.0 + t)
        AT[rows, :] = (hidden * cdf).astype(BF16)
        slope[rows, :] = cdf + hidden * (0.5 * (1.0 - t * t)) * (
            gelu_k * (1.0 + (3.0 * 0.044715) * square)
        )
        return carry

    received(recv_x, MAIN, E, 0)
    unpack(recv_x, X)
    lax.fori_loop(0, NZ, chunk_a, 0)
    received(recv_g, MAIN, E, 1)
    unpack(recv_g, G)
    gate_tile = recv_g[:, D + QD : D + QD + 128]
    rest_tile = dot(unpack_pick(0), gate_tile)
    gate_col = jnp.concatenate(
        [
            jnp.broadcast_to(gate_tile[:, 0:1].astype(F32), (S, 128)),
            jnp.broadcast_to(rest_tile[:, 64:65], (R, 128)),
        ],
        axis=0,
    )
    SG[...] = (gate_col[:, 0:1] * G[...].astype(F32)).astype(BF16)

    def chunk_b(c):
        rows = pl.ds(pl.multiple_of(c * FC, FC), FC)
        back = dot_nt(w_out[rows, :], G[...])
        HT[rows, :] = ((growr[0:1, :] * back) * slope[rows, :]).astype(BF16)
        gt[0:1, :] += jnp.sum(back * AT[rows, :].astype(F32), axis=0, keepdims=True)

    def at_offset(o):
        return lax.rem(z + o + 2 * NZ, NZ)

    def line_copy(src, buf, s, h, to, k):
        i = s * NSUB + h
        return pltpu.make_async_remote_copy(
            src_ref=src,
            dst_ref=buf.at[pl.ds(pl.multiple_of(i * SUB, SUB), SUB)],
            send_sem=ring_sem.at[2 * k, i],
            recv_sem=ring_sem.at[2 * k + 1, i],
            device_id=(me, to),
            device_id_type=MESH,
        )

    ways = ((AT, SG, cw0, cw, -1), (HT, X, ccw0, ccw, 1))

    def product(s, k):
        left, right, _, _, sign = ways[k]
        rows = pl.ds(pl.multiple_of(at_offset(sign * (1 + s)) * FC, FC), FC)
        own[k * FC : (k + 1) * FC, :] = dot(left[rows, :], right[...])

    def own_piece(k, h):
        return own[pl.ds(pl.multiple_of(k * FC + h * SUB, SUB), SUB), :]

    def ring_first(k):
        _, _, buf0, buf, sign = ways[k]

        def body(h, c):
            place_at = buf0.at[pl.ds(pl.multiple_of(h * SUB, SUB), SUB)]
            place_at[...] = own_piece(k, h).astype(BF16)
            line_copy(place_at, buf, 0, h, at_offset(-sign), k).start()
            return c

        lax.fori_loop(0, NSUB, body, 0)

    def ring_step(s):
        def body(h, c):
            for k, (_, _, _, buf, sign) in enumerate(ways):
                i = (s - 1) * NSUB + h
                place_at = buf.at[pl.ds(pl.multiple_of(i * SUB, SUB), SUB)]
                wait_bytes(place_at, ring_sem.at[2 * k + 1, i])
                place_at[...] = (own_piece(k, h) + place_at[...].astype(F32)).astype(BF16)
                line_copy(place_at, buf, s, h, at_offset(-sign), k).start()
            return c

        lax.fori_loop(0, NSUB, body, 0)

    def ring_end():
        outs = (wo, wiT)

        def body(h, c):
            for k, (_, _, _, buf, _) in enumerate(ways):
                i = (NZ - 2) * NSUB + h
                last = buf.at[pl.ds(pl.multiple_of(i * SUB, SUB), SUB)]
                wait_bytes(last, ring_sem.at[2 * k + 1, i])
                here = pl.ds(pl.multiple_of(h * SUB, SUB), SUB)
                outs[k][here, :] = (own_piece(k, h) + last[...].astype(F32)).astype(BF16)
            return c

        lax.fori_loop(0, NSUB, body, 0)

    def backs(lo, hi):
        def body(i, c):
            chunk_b(at_offset(i))
            return c

        lax.fori_loop(lo, hi, body, 0)

    def stats_on():
        received(sr1, 8, E, 2)
        total = sr1[0:8, :]
        for j in range(1, E):
            total += sr1[j * 8 : (j + 1) * 8, :]
        ss2[...] = total
        to_line(ss2, sr2, 8, 3)
        own_block(ss2, False, sr2, z, 8)

    def rows_home():
        def body(i, c):
            rows = pl.ds(pl.multiple_of(i * QD, QD), QD)
            rbT[rows, :] = dot(w_in[rows, :], HT[...]).astype(BF16)
            return c

        lax.fori_loop(0, SPLIT, body, 0)
        eye_s = hot(iota((S, S), 0) == iota((S, S), 1))
        rest = jnp.zeros((S, QD), F32)
        for q in range(SPLIT):
            cols = slice(q * QD, (q + 1) * QD)
            send_b[:, cols] = dot_nt(eye_s, rbT[cols, 0:S]).astype(BF16)
            rest += dot_nt(pack_pick(q), rbT[cols, S:ROWS])
        send_b[:, D : D + QD] = rest.astype(BF16)
        terms = jnp.broadcast_to(gt[0:1, :], (128, ROWS)).astype(BF16)
        r = iota((S, R), 1)
        s_ = iota((S, R), 0)
        any_pick = hot((s_ // MAIN == r // REST) & (lax.rem(s_, REST) == lax.rem(r, REST)))
        term_main = dot_nt(eye_s, terms[:, 0:S])
        term_rest = dot_nt(any_pick, terms[:, S:ROWS])
        send_b[:, D + QD : D + QD + 128] = jnp.where(
            iota((S, 128), 1) < 64, term_main, term_rest
        ).astype(BF16)
        to_plane(send_b, True, recv_b, MAIN, 4)
        own_block(send_b, True, recv_b, me, MAIN)

    def spread_grad(v):
        average = jnp.mean(v, axis=0, keepdims=True)
        dev = jnp.mean((v - average) ** 2, axis=0, keepdims=True)
        return (2.0 * (v - average) - 2.0 * dev / average) / (E * average * average)

    def at_home():
        received(sr2, 8, NZ, 3)
        received(recv_b, MAIN, E, 4)
        total = sr2[0:8, :]
        for j in range(1, NZ):
            total += sr2[j * 8 : (j + 1) * 8, :]
        row = jnp.broadcast_to(total[0:1, :], (E, 128))
        imp = jnp.sum(jnp.where(lane_id == row_id, row, 0.0), axis=1, keepdims=True)
        ld = jnp.sum(jnp.where(lane_id == row_id + E, row, 0.0), axis=1, keepdims=True)
        imp_coef = TOTAL * spread_grad(imp)
        load_coef = TOTAL * spread_grad(ld)
        probs = probs_s[...]
        zscore = z_s[...]
        tile = recv_b[:, D + QD : D + QD + 128].astype(F32)
        weighted = sel[...].astype(F32) * tile[:, 0:1] + selr[0:S, :].astype(F32) * tile[:, 64:65]
        gather = hot(iota((E, S), 1) // MAIN == iota((E, S), 0))
        score = dot(gather, weighted.astype(BF16)) + imp_coef
        noisy_grad = probs * (score - jnp.sum(probs * score, axis=0, keepdims=True))
        z_grad = load_coef * inv_root_tau * jnp.exp(-0.5 * zscore * zscore)
        thresh = thr[...] == iota((E, T), 0)
        logit_grad = (
            noisy_grad
            + z_grad
            - jnp.where(thresh, jnp.sum(z_grad, axis=0, keepdims=True), 0.0)
        )
        low = logit_grad.astype(BF16)
        llT_s[...] = low
        weight_part = dot(low, patches[...])
        bias_col = jnp.sum(logit_grad, axis=1, keepdims=True)
        bias_row = jnp.sum(jnp.where(lane_id == row_id, bias_col, 0.0), axis=0, keepdims=True)
        bias_tile = jnp.broadcast_to(bias_row, (8, 128))
        tiles = D // 128
        for p in range(E):
            a, b = p // tiles, p % tiles
            ws1[p * 16 : p * 16 + 8, :] = weight_part[a * 8 : a * 8 + 8, b * 128 : b * 128 + 128]
            ws1[p * 16 + 8 : p * 16 + 16, :] = bias_tile
        to_plane(ws1, True, wr1, 16, 5)
        own_block(ws1, True, wr1, me, 16)
        low_rows = dot_nt(eye_t, llT_s[...]).astype(BF16)
        for q in range(SPLIT):
            cols = slice(q * QD, (q + 1) * QD)
            out = dot(selT[...], recv_b[:, cols])
            out += dot(selrT[pl.ds(q * T, T), :], recv_b[:, D : D + QD])
            out += dot(low_rows, rwT[:, cols])
            pg[:, cols] = out.astype(BF16)

    def reduce_plane():
        received(wr1, 16, E, 5)
        total = wr1[0:16, :]
        for j in range(1, E):
            total += wr1[j * 16 : (j + 1) * 16, :]
        ws2[...] = total
        to_line(ws2, wr2, 16, 6)
        own_block(ws2, False, wr2, z, 16)

    def reduce_line():
        received(wr2, 16, NZ, 6)
        total = wr2[0:16, :]
        for j in range(1, NZ):
            total += wr2[j * 16 : (j + 1) * 16, :]
        rb[...] = total[8:16, :]
        ws3[...] = total[0:8, :]
        to_plane(ws3, False, wr3, 8, 7)
        own_block(ws3, False, wr3, me, 8)

    def spread_total():
        received(wr3, 8, E, 7)
        tiles = D // 128
        for p in range(E):
            a, b = p // tiles, p % tiles
            rgT[a * 8 : a * 8 + 8, b * 128 : b * 128 + 128] = wr3[p * 8 : p * 8 + 8, :]

    works = (rows_home, at_home, reduce_plane, reduce_line, spread_total)
    gaps = dict(zip((2, 4, 5, 6), works)) if NZ == 8 else {}
    product(0, 0)
    ring_first(0)
    growr[...] = dot_nt(hot(iota((8, 128), 1) == 0), gate_col.astype(BF16))
    gt[...] = jnp.zeros_like(gt)
    backs(1, 2)
    product(0, 1)
    ring_first(1)
    half = NZ // 2
    for s in range(NZ - 1):
        if s > 0:
            ring_step(s)
        if s == 0:
            backs(2, half + 1)
        if s == 1 or NZ == 2:
            backs(half + 1, NZ + 1)
        product(s + 1, 0)
        product(s + 1, 1)
        if s == 1 or NZ == 2:
            stats_on()
        if s in gaps:
            gaps[s]()
    ring_end()
    for work in works[len(gaps):]:
        work()

    sent(recv_x, MAIN, E, 0)
    sent(recv_g, MAIN, E, 1)
    sent(sr1, 8, E, 2)
    sent(sr2, 8, NZ, 3)
    sent(recv_b, MAIN, E, 4)
    sent(wr1, 16, E, 5)
    sent(wr2, 16, NZ, 6)
    sent(wr3, 8, E, 7)

    def drain(i, c):
        for k, way in enumerate(ways):
            wait_bytes(way[2].at[pl.ds(0, SUB)], ring_sem.at[2 * k, i])
        return c

    lax.fori_loop(0, (NZ - 1) * NSUB, drain, 0)


def finish(pg, wiT, wo, rgT, rb, pg_out, wi_out, wo_out, rgT_out, rb_out):
    pg_out[...] = pg[...]
    wi_out[...] = wiT[...].T
    wo_out[...] = wo[...]
    rgT_out[...] = rgT[...]
    rb_out[...] = rb[0:1, 0 : rb_out.shape[1]]


def on_device(
    patches, router_weight, router_bias, noise, top_experts, threshold_expert, w_in, w_out, out_grad
):
    T, D = patches.shape
    E = router_weight.shape[1]
    NZ = lax.axis_size("dp")
    F = w_in.shape[2]
    FC = F // NZ
    S = E * MAIN
    ROWS = S + E * REST
    QD = D // SPLIT
    WX = D + QD
    WG = WX + 128
    VMEM = pltpu.VMEM
    whole = pl.BlockSpec(memory_space=pltpu.VMEM)
    far = pl.BlockSpec(memory_space=pl.ANY)
    pg, wiT, wo, rgT, rb = pl.pallas_call(
        functools.partial(kernel, E, NZ, float(T * E * NZ)),
        out_shape=(
            jax.ShapeDtypeStruct((T, D), BF16),
            jax.ShapeDtypeStruct((FC, D), BF16),
            jax.ShapeDtypeStruct((FC, D), BF16),
            jax.ShapeDtypeStruct((E, D), F32),
            jax.ShapeDtypeStruct((8, 128), F32),
        ),
        in_specs=[far] + [whole] * 5 + [far] * 3,
        out_specs=(whole,) * 5,
        scratch_shapes=[
            VMEM((T, D), BF16), VMEM((T, D), BF16),
            VMEM((D, F), BF16), VMEM((F, D), BF16), VMEM((F, D), BF16),
            VMEM((SPLIT * E * REST, S), BF16), VMEM((F, ROWS), F32), VMEM((2 * FC, D), F32),
            VMEM((S, T), BF16), VMEM((SPLIT * S, T), BF16),
            VMEM((T, S), BF16), VMEM((SPLIT * T, S), BF16),
            VMEM((S, WX), BF16), VMEM((S, WG), BF16), VMEM((S, WX), BF16), VMEM((S, WG), BF16),
            VMEM((S, WG), BF16), VMEM((S, WG), BF16),
            VMEM((ROWS, D), BF16), VMEM((ROWS, D), BF16), VMEM((ROWS, D), BF16),
            VMEM((F, ROWS), BF16), VMEM((F, ROWS), BF16), VMEM((D, ROWS), BF16),
            VMEM((8, ROWS), F32), VMEM((8, ROWS), F32),
            VMEM((FC, D), BF16), VMEM(((NZ - 1) * FC, D), BF16),
            VMEM((FC, D), BF16), VMEM(((NZ - 1) * FC, D), BF16),
            VMEM((E, T), F32), VMEM((E, T), F32), VMEM((E, T), BF16),
            VMEM((8, 128), F32), VMEM((E * 8, 128), F32),
            VMEM((8, 128), F32), VMEM((NZ * 8, 128), F32),
            VMEM((E * 16, 128), F32), VMEM((E * 16, 128), F32),
            VMEM((16, 128), F32), VMEM((NZ * 16, 128), F32),
            VMEM((8, 128), F32), VMEM((E * 8, 128), F32),
            pltpu.SemaphoreType.DMA((4,)),
            pltpu.SemaphoreType.DMA((16,)),
            pltpu.SemaphoreType.DMA((4, (NZ - 1) * NSUB)),
        ],
        compiler_params=pltpu.CompilerParams(
            collective_id=0, has_side_effects=True, vmem_limit_bytes=63 * 1024 * 1024
        ),
        name="moe_back",
    )(
        patches,
        router_weight.T,
        router_bias.reshape(1, E),
        noise.T,
        top_experts.T,
        threshold_expert.reshape(1, T),
        out_grad,
        w_in[0],
        w_out[0],
    )
    pg, wi, wo, rgT, rb = pl.pallas_call(
        finish,
        out_shape=(
            jax.ShapeDtypeStruct((T, D), BF16),
            jax.ShapeDtypeStruct((D, FC), BF16),
            jax.ShapeDtypeStruct((FC, D), BF16),
            jax.ShapeDtypeStruct((E, D), F32),
            jax.ShapeDtypeStruct((1, E), F32),
        ),
        in_specs=[whole] * 5,
        out_specs=(whole,) * 5,
        name="moe_back_out",
    )(pg, wiT, wo, rgT, rb)
    return (pg, wi[None], wo[None], rgT.T, rb[0])


def solution(mesh):
    both = ("expert", "dp")
    in_specs = (
        P(both, None), P(), P(), P(both, None), P(both, None), P(both),
        P("expert", None, None), P("expert", None, None), P(both, None),
    )
    out_specs = (P(both, None), P("expert", None, "dp"), P("expert", "dp", None), P(), P())
    return jax.shard_map(
        on_device, mesh=mesh, in_specs=in_specs, out_specs=out_specs, check_vma=False
    )
```

```python
import functools
import math

import jax
import jax.numpy as jnp
from jax import lax
from jax.experimental import pallas as pl
from jax.experimental.pallas import tpu as pltpu
from jax.sharding import PartitionSpec as P

F32 = jnp.float32
BF16 = jnp.bfloat16
MESH = pl.DeviceIdType.MESH
MAIN = 16
REST = 4
SPLIT = 4
NSUB = 4
inv_root_two = 0.7071067811865476
inv_root_tau = 0.3989422804014327
gelu_k = math.sqrt(2.0 / math.pi)


def dot(a, b):
    return jnp.dot(a, b, preferred_element_type=F32)


def dot_nt(a, b):
    return lax.dot_general(a, b, (((1,), (1,)), ((), ())), preferred_element_type=F32)


def iota(shape, dim):
    return lax.broadcasted_iota(jnp.int32, shape, dim)


def hot(mask):
    return jnp.where(mask, 1.0, 0.0).astype(BF16)


def wait_bytes(ref, sem):
    pltpu.make_async_copy(ref, ref, sem).wait()


def kernel(
    E, NZ, TOTAL,
    patches_hbm, rwT, bias, noiseT, topT, thr, og_hbm, w_in_hbm, w_out_hbm,
    pg, wiT, wo, rgT, rb,
    patches, og, w_in, w_out, w_inT, picks, slope, own, sel, selr, selT, selrT, send_x, send_g, recv_x, recv_g,
    recv_b, X, G, SG, AT, HT, growr, gt, cw, ccw,
    probs_s, z_s, llT_s, stat, sr1, ss2, sr2, ws1, wr1, ws2, wr2, ws3, wr3, wsem, px, ring_sem,
):
    T, D = patches.shape
    F = w_out.shape[0]
    FC = F // NZ
    SUB = FC // NSUB
    QD = D // SPLIT
    S = E * MAIN
    R = E * REST
    ROWS = S + R
    me = lax.axis_index("expert")
    z = lax.axis_index("dp")

    load_patches = pltpu.make_async_copy(patches_hbm, patches, wsem.at[2])
    load_og = pltpu.make_async_copy(og_hbm, og, wsem.at[3])
    load_patches.start()
    load_og.start()
    load_in = pltpu.make_async_copy(w_in_hbm, w_in, wsem.at[0])
    load_out = pltpu.make_async_copy(w_out_hbm, w_out, wsem.at[1])
    load_in.start()
    load_out.start()

    barrier = pltpu.get_barrier_semaphore()

    def greet_plane(p, c):
        pl.semaphore_signal(
            barrier, inc=1, device_id=(lax.rem(me + p, E), z), device_id_type=MESH
        )
        return c

    def greet_line(p, c):
        pl.semaphore_signal(
            barrier, inc=1, device_id=(me, lax.rem(z + p, NZ)), device_id_type=MESH
        )
        return c

    lax.fori_loop(1, E, greet_plane, 0)
    lax.fori_loop(1, NZ, greet_line, 0)

    NX = E // 8
    offsets = [(a, b, c) for a in range(NX) for b in range(4) for c in range(2)][1:]
    offsets.sort(key=lambda o: -(min(o[0], NX - o[0]) + min(o[1], 4 - o[1])))
    my_x, my_y, my_c = me // 8, lax.rem(me // 2, 4), lax.rem(me, 2)
    turn_of = 1 - 2 * my_c

    def to_plane_far(src, dst, rows, k):
        for a, b, c in offsets:
            peer = (
                lax.rem(my_x + turn_of * a + NX, NX) * 8
                + lax.rem(my_y + turn_of * b + 4, 4) * 2
                + lax.rem(my_c + c, 2)
            )
            pltpu.make_async_remote_copy(
                src_ref=src.at[pl.ds(pl.multiple_of(peer * rows, rows), rows)],
                dst_ref=dst.at[pl.ds(pl.multiple_of(me * rows, rows), rows)],
                send_sem=px.at[2 * k],
                recv_sem=px.at[2 * k + 1],
                device_id=(peer, z),
                device_id_type=MESH,
            ).start()

    def to_plane(src, by_peer, dst, rows, k):
        def body(i, c):
            half = (i + 1) // 2
            p = half + (1 - lax.rem(i, 2)) * (E - 2 * half)
            peer = lax.rem(me + p, E)
            if by_peer:
                piece = src.at[pl.ds(pl.multiple_of(peer * rows, rows), rows)]
            else:
                piece = src
            pltpu.make_async_remote_copy(
                src_ref=piece,
                dst_ref=dst.at[pl.ds(pl.multiple_of(me * rows, rows), rows)],
                send_sem=px.at[2 * k],
                recv_sem=px.at[2 * k + 1],
                device_id=(peer, z),
                device_id_type=MESH,
            ).start()
            return c

        lax.fori_loop(1, E, body, 0)

    def to_line(src, dst, rows, k):
        def body(p, c):
            pltpu.make_async_remote_copy(
                src_ref=src,
                dst_ref=dst.at[pl.ds(pl.multiple_of(z * rows, rows), rows)],
                send_sem=px.at[2 * k],
                recv_sem=px.at[2 * k + 1],
                device_id=(me, lax.rem(z + p, NZ)),
                device_id_type=MESH,
            ).start()
            return c

        lax.fori_loop(1, NZ, body, 0)

    def own_block(src, by_peer, dst, at, rows):
        here = pl.ds(pl.multiple_of(at * rows, rows), rows)
        dst[here, :] = src[here, :] if by_peer else src[...]

    def received(dst, rows, peers, k):
        wait_bytes(dst.at[pl.ds(0, (peers - 1) * rows)], px.at[2 * k + 1])

    def sent(dst, rows, peers, k):
        wait_bytes(dst.at[pl.ds(0, (peers - 1) * rows)], px.at[2 * k])

    experts = iota((E, T), 0)
    member = (topT[0:1, :] == experts) | (topT[1:2, :] == experts)
    earlier = hot(iota((T, T), 0) < iota((T, T), 1))
    before = dot(hot(member), earlier)
    code = jnp.where(member, before, -1.0).astype(BF16)
    spread = hot(iota((S, E), 0) // MAIN == iota((S, E), 1))
    code_rows = dot(spread, code)
    place = lax.rem(iota((S, T), 0), MAIN)
    sel[...] = hot(code_rows == place.astype(F32))
    is_rest = code_rows == (lax.rem(place, REST) + MAIN).astype(F32)
    for q in range(SPLIT):
        selr[pl.ds(q * S, S), :] = hot(is_rest & (place // REST == q))

    RB = min(S, 128)

    def pack_rows(src, dst):
        def body(i, c):
            rows = pl.ds(pl.multiple_of(i * RB, RB), RB)
            dst[rows, 0:D] = dot(sel[rows, :], src[...]).astype(BF16)
            acc = jnp.zeros((RB, QD), F32)
            for q in range(SPLIT):
                pick = selr[pl.ds(pl.multiple_of(q * S + i * RB, RB), RB), :]
                acc += dot(pick, src[:, q * QD : (q + 1) * QD])
            dst[rows, D : D + QD] = acc.astype(BF16)
            return c

        lax.fori_loop(0, S // RB, body, 0)

    load_patches.wait()
    pack_rows(patches, send_x)
    pl.semaphore_wait(barrier, E + NZ - 2)
    to_plane_far(send_x, recv_x, MAIN, 0)
    own_block(send_x, True, recv_x, me, MAIN)

    bias_pick = iota((E, E), 0) == iota((E, E), 1)
    bias_rows = jnp.sum(jnp.where(bias_pick, bias[...], 0.0), axis=1, keepdims=True)
    logits = dot_nt(rwT[...], patches[...]) + bias_rows
    noisy = logits + noiseT[...]
    top = jnp.max(noisy, axis=0, keepdims=True)
    powers = jnp.exp(noisy - top)
    probs = powers / jnp.sum(powers, axis=0, keepdims=True)
    thresh = thr[...] == experts
    base = jnp.sum(jnp.where(thresh, noisy, 0.0), axis=0, keepdims=True)
    zscore = logits - base
    probs_s[...] = probs
    z_s[...] = zscore
    prob_rows = dot(spread, probs.astype(BF16))
    gate_main = jnp.sum(prob_rows * sel[...].astype(F32), axis=1, keepdims=True)
    gate_rest = jnp.sum(jnp.where(is_rest, prob_rows, 0.0), axis=1, keepdims=True)
    low_lanes = iota((S, 128), 1) < 64
    send_g[:, D + QD : D + QD + 128] = jnp.where(low_lanes, gate_main, gate_rest).astype(BF16)
    load_og.wait()
    pack_rows(og, send_g)
    to_plane_far(send_g, recv_g, MAIN, 1)
    own_block(send_g, True, recv_g, me, MAIN)

    importance = jnp.sum(probs, axis=1, keepdims=True)
    load = jnp.sum(0.5 * (1.0 + lax.erf(zscore * inv_root_two)), axis=1, keepdims=True)
    row_id = iota((E, 128), 0)
    lane_id = iota((E, 128), 1)
    both = jnp.where(lane_id == row_id, importance, 0.0) + jnp.where(
        lane_id == row_id + E, load, 0.0
    )
    stat[...] = jnp.broadcast_to(jnp.sum(both, axis=0, keepdims=True), (8, 128))
    to_plane(stat, False, sr1, 8, 2)
    own_block(stat, False, sr1, me, 8)

    eye_t = hot(iota((T, T), 0) == iota((T, T), 1))
    selT[...] = dot_nt(eye_t, sel[...]).astype(BF16)
    for q in range(SPLIT):
        selrT[pl.ds(q * T, T), :] = dot_nt(eye_t, selr[pl.ds(q * S, S), :]).astype(BF16)
    for q in range(SPLIT):
        r = iota((R, S), 0)
        picks[pl.ds(q * R, R), :] = hot(
            iota((R, S), 1) == (r // REST) * MAIN + q * REST + lax.rem(r, REST)
        )
    load_in.wait()
    load_out.wait()

    def turn(i, c):
        cols = pl.ds(pl.multiple_of(i * 256, 256), 256)
        w_inT[cols, :] = w_in[:, cols].T
        return c

    lax.fori_loop(0, F // 256, turn, 0)

    def unpack_pick(q):
        return picks[pl.ds(q * R, R), :]

    def pack_pick(q):
        r = iota((S, R), 1)
        return hot(iota((S, R), 0) == (r // REST) * MAIN + q * REST + lax.rem(r, REST))

    def unpack(src, dst):
        dst[0:S, :] = src[:, 0:D]
        for q in range(SPLIT):
            dst[S:ROWS, q * QD : (q + 1) * QD] = dot(
                unpack_pick(q), src[:, D : D + QD]
            ).astype(BF16)

    def chunk_a(c, carry):
        rows = pl.ds(pl.multiple_of(c * FC, FC), FC)
        hidden = dot_nt(w_inT[rows, :], X[...])
        square = hidden * hidden
        t = jnp.tanh(gelu_k * (hidden + 0.044715 * (square * hidden)))
        cdf = 0.5 * (1.0 + t)
        AT[rows, :] = (hidden * cdf).astype(BF16)
        slope[rows, :] = cdf + hidden * (0.5 * (1.0 - t * t)) * (
            gelu_k * (1.0 + (3.0 * 0.044715) * square)
        )
        return carry

    received(recv_x, MAIN, E, 0)
    unpack(recv_x, X)
    lax.fori_loop(0, NZ, chunk_a, 0)
    received(recv_g, MAIN, E, 1)
    for q in range(SPLIT):
        G[S:ROWS, q * QD : (q + 1) * QD] = dot(
            unpack_pick(q), recv_g[:, D : D + QD]
        ).astype(BF16)
    gate_tile = recv_g[:, D + QD : D + QD + 128]
    rest_tile = dot(unpack_pick(0), gate_tile)
    gate_main = gate_tile[:, 0:1].astype(F32)
    gate_rest = rest_tile[:, 64:65]
    SG[0:S, :] = (gate_main * recv_g[:, 0:D].astype(F32)).astype(BF16)
    SG[S:ROWS, :] = (gate_rest * G[S:ROWS, :].astype(F32)).astype(BF16)

    def chunk_b(c):
        rows = pl.ds(pl.multiple_of(c * FC, FC), FC)
        back = dot_nt(w_out[rows, :], G[...])
        HT[rows, :] = ((growr[0:1, :] * back) * slope[rows, :]).astype(BF16)
        gt[0:1, :] += jnp.sum(back * AT[rows, :].astype(F32), axis=0, keepdims=True)

    def at_offset(o):
        return lax.rem(z + o + 2 * NZ, NZ)

    def line_copy(src, buf, s, h, to, k):
        i = s * NSUB + h
        return pltpu.make_async_remote_copy(
            src_ref=src,
            dst_ref=buf.at[pl.ds(pl.multiple_of(i * SUB, SUB), SUB)],
            send_sem=ring_sem.at[2 * k, i],
            recv_sem=ring_sem.at[2 * k + 1, i],
            device_id=(me, to),
            device_id_type=MESH,
        )

    cw0, ccw0 = w_inT.at[pl.ds(0, FC)], w_inT.at[pl.ds(FC, FC)]
    rbT = w_inT.at[pl.ds(F // 2, D), 0:ROWS]
    send_b = send_g
    ways = ((AT, SG, cw0, cw, -1), (HT, X, ccw0, ccw, 1))

    def product(s, k):
        left, right, _, _, sign = ways[k]
        rows = pl.ds(pl.multiple_of(at_offset(sign * (1 + s)) * FC, FC), FC)
        own[k * FC : (k + 1) * FC, :] = dot(left[rows, :], right[...])

    def own_piece(k, h):
        return own[pl.ds(pl.multiple_of(k * FC + h * SUB, SUB), SUB), :]

    def ring_first(k):
        _, _, buf0, buf, sign = ways[k]

        def body(h, c):
            place_at = buf0.at[pl.ds(pl.multiple_of(h * SUB, SUB), SUB)]
            place_at[...] = own_piece(k, h).astype(BF16)
            line_copy(place_at, buf, 0, h, at_offset(-sign), k).start()
            return c

        lax.fori_loop(0, NSUB, body, 0)

    def ring_step(s):
        def body(h, c):
            for k, (_, _, _, buf, sign) in enumerate(ways):
                i = (s - 1) * NSUB + h
                place_at = buf.at[pl.ds(pl.multiple_of(i * SUB, SUB), SUB)]
                wait_bytes(place_at, ring_sem.at[2 * k + 1, i])
                place_at[...] = (own_piece(k, h) + place_at[...].astype(F32)).astype(BF16)
                line_copy(place_at, buf, s, h, at_offset(-sign), k).start()
            return c

        lax.fori_loop(0, NSUB, body, 0)

    def ring_end():
        outs = (wo, wiT)

        def body(h, c):
            for k, (_, _, _, buf, _) in enumerate(ways):
                i = (NZ - 2) * NSUB + h
                last = buf.at[pl.ds(pl.multiple_of(i * SUB, SUB), SUB)]
                wait_bytes(last, ring_sem.at[2 * k + 1, i])
                here = pl.ds(pl.multiple_of(h * SUB, SUB), SUB)
                outs[k][here, :] = (own_piece(k, h) + last[...].astype(F32)).astype(BF16)
            return c

        lax.fori_loop(0, NSUB, body, 0)

    def backs(lo, hi):
        def body(i, c):
            chunk_b(at_offset(i))
            return c

        lax.fori_loop(lo, hi, body, 0)

    def stats_on():
        received(sr1, 8, E, 2)
        total = sr1[0:8, :]
        for j in range(1, E):
            total += sr1[j * 8 : (j + 1) * 8, :]
        ss2[...] = total
        to_line(ss2, sr2, 8, 3)
        own_block(ss2, False, sr2, z, 8)

    def rows_home():
        def body(i, c):
            rows = pl.ds(pl.multiple_of(i * QD, QD), QD)
            rbT[rows, :] = dot(w_in[rows, :], HT[...]).astype(BF16)
            return c

        lax.fori_loop(0, SPLIT, body, 0)
        sent(recv_g, MAIN, E, 1)
        eye_s = hot(iota((S, S), 0) == iota((S, S), 1))
        rest = jnp.zeros((S, QD), F32)
        for q in range(SPLIT):
            cols = slice(q * QD, (q + 1) * QD)
            send_b[:, cols] = dot_nt(eye_s, rbT[cols, 0:S]).astype(BF16)
            rest += dot_nt(pack_pick(q), rbT[cols, S:ROWS])
        send_b[:, D : D + QD] = rest.astype(BF16)
        terms = jnp.broadcast_to(gt[0:1, :], (128, ROWS)).astype(BF16)
        r = iota((S, R), 1)
        s_ = iota((S, R), 0)
        any_pick = hot((s_ // MAIN == r // REST) & (lax.rem(s_, REST) == lax.rem(r, REST)))
        term_main = dot_nt(eye_s, terms[:, 0:S])
        term_rest = dot_nt(any_pick, terms[:, S:ROWS])
        send_b[:, D + QD : D + QD + 128] = jnp.where(
            iota((S, 128), 1) < 64, term_main, term_rest
        ).astype(BF16)
        to_plane_far(send_b, recv_b, MAIN, 4)
        own_block(send_b, True, recv_b, me, MAIN)

    def spread_grad(v):
        average = jnp.mean(v, axis=0, keepdims=True)
        dev = jnp.mean((v - average) ** 2, axis=0, keepdims=True)
        return (2.0 * (v - average) - 2.0 * dev / average) / (E * average * average)

    def at_home():
        received(sr2, 8, NZ, 3)
        received(recv_b, MAIN, E, 4)
        total = sr2[0:8, :]
        for j in range(1, NZ):
            total += sr2[j * 8 : (j + 1) * 8, :]
        row = jnp.broadcast_to(total[0:1, :], (E, 128))
        imp = jnp.sum(jnp.where(lane_id == row_id, row, 0.0), axis=1, keepdims=True)
        ld = jnp.sum(jnp.where(lane_id == row_id + E, row, 0.0), axis=1, keepdims=True)
        imp_coef = TOTAL * spread_grad(imp)
        load_coef = TOTAL * spread_grad(ld)
        probs = probs_s[...]
        zscore = z_s[...]
        tile = recv_b[:, D + QD : D + QD + 128].astype(F32)
        weighted = sel[...].astype(F32) * tile[:, 0:1] + selr[0:S, :].astype(F32) * tile[:, 64:65]
        gather = hot(iota((E, S), 1) // MAIN == iota((E, S), 0))
        score = dot(gather, weighted.astype(BF16)) + imp_coef
        noisy_grad = probs * (score - jnp.sum(probs * score, axis=0, keepdims=True))
        z_grad = load_coef * inv_root_tau * jnp.exp(-0.5 * zscore * zscore)
        thresh = thr[...] == iota((E, T), 0)
        logit_grad = (
            noisy_grad
            + z_grad
            - jnp.where(thresh, jnp.sum(z_grad, axis=0, keepdims=True), 0.0)
        )
        low = logit_grad.astype(BF16)
        llT_s[...] = low
        weight_part = dot(low, patches[...])
        bias_col = jnp.sum(logit_grad, axis=1, keepdims=True)
        bias_row = jnp.sum(jnp.where(lane_id == row_id, bias_col, 0.0), axis=0, keepdims=True)
        bias_tile = jnp.broadcast_to(bias_row, (8, 128))
        tiles = D // 128
        for p in range(E):
            a, b = p // tiles, p % tiles
            ws1[p * 16 : p * 16 + 8, :] = weight_part[a * 8 : a * 8 + 8, b * 128 : b * 128 + 128]
            ws1[p * 16 + 8 : p * 16 + 16, :] = bias_tile
        to_plane(ws1, True, wr1, 16, 5)
        own_block(ws1, True, wr1, me, 16)
        low_rows = dot_nt(eye_t, llT_s[...]).astype(BF16)
        for q in range(SPLIT):
            cols = slice(q * QD, (q + 1) * QD)
            out = dot(selT[...], recv_b[:, cols])
            out += dot(selrT[pl.ds(q * T, T), :], recv_b[:, D : D + QD])
            out += dot(low_rows, rwT[:, cols])
            pg[:, cols] = out.astype(BF16)

    def reduce_plane():
        received(wr1, 16, E, 5)
        total = wr1[0:16, :]
        for j in range(1, E):
            total += wr1[j * 16 : (j + 1) * 16, :]
        ws2[...] = total
        to_line(ws2, wr2, 16, 6)
        own_block(ws2, False, wr2, z, 16)

    def reduce_line():
        received(wr2, 16, NZ, 6)
        total = wr2[0:16, :]
        for j in range(1, NZ):
            total += wr2[j * 16 : (j + 1) * 16, :]
        rb[...] = total[8:16, :]
        ws3[...] = total[0:8, :]
        to_plane(ws3, False, wr3, 8, 7)
        own_block(ws3, False, wr3, me, 8)

    def spread_total():
        received(wr3, 8, E, 7)
        tiles = D // 128
        for p in range(E):
            a, b = p // tiles, p % tiles
            rgT[a * 8 : a * 8 + 8, b * 128 : b * 128 + 128] = wr3[p * 8 : p * 8 + 8, :]

    works = (rows_home, at_home, reduce_plane, reduce_line, spread_total)
    gaps = dict(zip((2, 4, 5, 6), works)) if NZ == 8 else {}
    product(0, 0)
    ring_first(0)
    G[0:S, :] = recv_g[:, 0:D]
    first_lane = hot(iota((8, 128), 1) == 0)
    last_lane = hot(iota((8, 128), 1) == 64)
    growr[:, 0:S] = dot_nt(first_lane, gate_tile)
    growr[:, S:ROWS] = dot_nt(last_lane, rest_tile.astype(BF16))
    gt[...] = jnp.zeros_like(gt)
    backs(1, 2)
    product(0, 1)
    ring_first(1)
    half = NZ // 2
    for s in range(NZ - 1):
        if s > 0:
            ring_step(s)
        if s == 0:
            backs(2, half + 1)
        if s == 1 or NZ == 2:
            backs(half + 1, NZ + 1)
        product(s + 1, 0)
        product(s + 1, 1)
        if s == 1 or NZ == 2:
            stats_on()
        if s in gaps:
            gaps[s]()
    ring_end()
    for work in works[len(gaps):]:
        work()

    sent(recv_x, MAIN, E, 0)
    sent(sr1, 8, E, 2)
    sent(sr2, 8, NZ, 3)
    sent(recv_b, MAIN, E, 4)
    sent(wr1, 16, E, 5)
    sent(wr2, 16, NZ, 6)
    sent(wr3, 8, E, 7)

    def drain(i, c):
        for k, way in enumerate(ways):
            wait_bytes(way[2].at[pl.ds(0, SUB)], ring_sem.at[2 * k, i])
        return c

    lax.fori_loop(0, (NZ - 1) * NSUB, drain, 0)


def finish(pg, wiT, wo, rgT, rb, pg_out, wi_out, wo_out, rgT_out, rb_out):
    pg_out[...] = pg[...]
    wi_out[...] = wiT[...].T
    wo_out[...] = wo[...]
    rgT_out[...] = rgT[...]
    rb_out[...] = rb[0:1, 0 : rb_out.shape[1]]


def on_device(
    patches, router_weight, router_bias, noise, top_experts, threshold_expert, w_in, w_out, out_grad
):
    T, D = patches.shape
    E = router_weight.shape[1]
    NZ = lax.axis_size("dp")
    F = w_in.shape[2]
    FC = F // NZ
    S = E * MAIN
    ROWS = S + E * REST
    QD = D // SPLIT
    WX = D + QD
    WG = WX + 128
    VMEM = pltpu.VMEM
    whole = pl.BlockSpec(memory_space=pltpu.VMEM)
    far = pl.BlockSpec(memory_space=pl.ANY)
    pg, wiT, wo, rgT, rb = pl.pallas_call(
        functools.partial(kernel, E, NZ, float(T * E * NZ)),
        out_shape=(
            jax.ShapeDtypeStruct((T, D), BF16),
            jax.ShapeDtypeStruct((FC, D), BF16),
            jax.ShapeDtypeStruct((FC, D), BF16),
            jax.ShapeDtypeStruct((E, D), F32),
            jax.ShapeDtypeStruct((8, 128), F32),
        ),
        in_specs=[far] + [whole] * 5 + [far] * 3,
        out_specs=(whole,) * 5,
        scratch_shapes=[
            VMEM((T, D), BF16), VMEM((T, D), BF16),
            VMEM((D, F), BF16), VMEM((F, D), BF16), VMEM((F, D), BF16),
            VMEM((SPLIT * E * REST, S), BF16), VMEM((F, ROWS), F32), VMEM((2 * FC, D), F32),
            VMEM((S, T), BF16), VMEM((SPLIT * S, T), BF16),
            VMEM((T, S), BF16), VMEM((SPLIT * T, S), BF16),
            VMEM((S, WX), BF16), VMEM((S, WG), BF16), VMEM((S, WX), BF16), VMEM((S, WG), BF16),
            VMEM((S, WG), BF16),
            VMEM((ROWS, D), BF16), VMEM((ROWS, D), BF16), VMEM((ROWS, D), BF16),
            VMEM((F, ROWS), BF16), VMEM((F, ROWS), BF16),
            VMEM((8, ROWS), F32), VMEM((8, ROWS), F32),
            VMEM(((NZ - 1) * FC, D), BF16),
            VMEM(((NZ - 1) * FC, D), BF16),
            VMEM((E, T), F32), VMEM((E, T), F32), VMEM((E, T), BF16),
            VMEM((8, 128), F32), VMEM((E * 8, 128), F32),
            VMEM((8, 128), F32), VMEM((NZ * 8, 128), F32),
            VMEM((E * 16, 128), F32), VMEM((E * 16, 128), F32),
            VMEM((16, 128), F32), VMEM((NZ * 16, 128), F32),
            VMEM((8, 128), F32), VMEM((E * 8, 128), F32),
            pltpu.SemaphoreType.DMA((4,)),
            pltpu.SemaphoreType.DMA((16,)),
            pltpu.SemaphoreType.DMA((4, (NZ - 1) * NSUB)),
        ],
        compiler_params=pltpu.CompilerParams(
            collective_id=0, has_side_effects=True, vmem_limit_bytes=52 * 1024 * 1024
        ),
        name="moe_back",
    )(
        patches,
        router_weight.T,
        router_bias.reshape(1, E),
        noise.T,
        top_experts.T,
        threshold_expert.reshape(1, T),
        out_grad,
        w_in[0],
        w_out[0],
    )
    pg, wi, wo, rgT, rb = pl.pallas_call(
        finish,
        out_shape=(
            jax.ShapeDtypeStruct((T, D), BF16),
            jax.ShapeDtypeStruct((D, FC), BF16),
            jax.ShapeDtypeStruct((FC, D), BF16),
            jax.ShapeDtypeStruct((E, D), F32),
            jax.ShapeDtypeStruct((1, E), F32),
        ),
        in_specs=[whole] * 5,
        out_specs=(whole,) * 5,
        compiler_params=pltpu.CompilerParams(vmem_limit_bytes=8 * 1024 * 1024),
        name="moe_back_out",
    )(pg, wiT, wo, rgT, rb)
    return (pg, wi[None], wo[None], rgT.T, rb[0])


def solution(mesh):
    both = ("expert", "dp")
    in_specs = (
        P(both, None), P(), P(), P(both, None), P(both, None), P(both),
        P("expert", None, None), P("expert", None, None), P(both, None),
    )
    out_specs = (P(both, None), P("expert", None, "dp"), P("expert", "dp", None), P(), P())
    return jax.shard_map(
        on_device, mesh=mesh, in_specs=in_specs, out_specs=out_specs, check_vma=False
    )
```

```python
import functools
import math

import jax
import jax.numpy as jnp
from jax import lax
from jax.experimental import pallas as pl
from jax.experimental.pallas import tpu as pltpu
from jax.sharding import PartitionSpec as P

F32 = jnp.float32
BF16 = jnp.bfloat16
MESH = pl.DeviceIdType.MESH
MAIN = 16
REST = 4
SPLIT = 4
NSUB = 4
inv_root_two = 0.7071067811865476
inv_root_tau = 0.3989422804014327
gelu_k = math.sqrt(2.0 / math.pi)


def dot(a, b):
    return jnp.dot(a, b, preferred_element_type=F32)


def dot_nt(a, b):
    return lax.dot_general(a, b, (((1,), (1,)), ((), ())), preferred_element_type=F32)


def iota(shape, dim):
    return lax.broadcasted_iota(jnp.int32, shape, dim)


def hot(mask):
    return jnp.where(mask, 1.0, 0.0).astype(BF16)


def wait_bytes(ref, sem):
    pltpu.make_async_copy(ref, ref, sem).wait()


def kernel(
    E, NZ, TOTAL,
    patches_hbm, rwT_hbm, bias_hbm, noiseT_hbm, topT_hbm, thr_hbm, og_hbm, w_in_hbm, w_out_hbm,
    pg_hbm, wiT_hbm, wo_hbm, rgT_hbm, rb_hbm,
    pg, wiT, wo, rgT, rb, osem, sgate, rgate, rwT, bias, noiseT, topT, thr, patches, og, w_in, w_out, w_inT, picks, slope, own, sel, selr, selT, selrT, send_x, send_g, recv_x, recv_g,
    recv_b, X, G, SG, AT, HT, growr, gt, cw, ccw,
    probs_s, z_s, llT_s, stat, sr1, ss2, sr2, ws1, wr1, ws2, wr2, ws3, wr3, wsem, px, ring_sem,
):
    T, D = patches.shape
    F = w_out.shape[0]
    FC = F // NZ
    SUB = FC // NSUB
    QD = D // SPLIT
    S = E * MAIN
    R = E * REST
    ROWS = S + R
    me = lax.axis_index("expert")
    z = lax.axis_index("dp")

    load_patches = pltpu.make_async_copy(patches_hbm, patches, wsem.at[2])
    load_og = pltpu.make_async_copy(og_hbm, og, wsem.at[3])
    small = [
        pltpu.make_async_copy(a, b, wsem.at[4 + i])
        for i, (a, b) in enumerate(
            ((topT_hbm, topT), (rwT_hbm, rwT), (bias_hbm, bias), (noiseT_hbm, noiseT), (thr_hbm, thr))
        )
    ]
    small[0].start()
    load_patches.start()
    for load_small in small[1:]:
        load_small.start()
    load_og.start()
    load_in = pltpu.make_async_copy(w_in_hbm, w_in, wsem.at[0])
    load_out = pltpu.make_async_copy(w_out_hbm, w_out, wsem.at[1])
    load_in.start()
    load_out.start()

    barrier = pltpu.get_barrier_semaphore()

    def greet_plane(p, c):
        pl.semaphore_signal(
            barrier, inc=1, device_id=(lax.rem(me + p, E), z), device_id_type=MESH
        )
        return c

    def greet_line(p, c):
        pl.semaphore_signal(
            barrier, inc=1, device_id=(me, lax.rem(z + p, NZ)), device_id_type=MESH
        )
        return c

    lax.fori_loop(1, E, greet_plane, 0)
    lax.fori_loop(1, NZ, greet_line, 0)

    NX = E // 8
    offsets = [(a, b, c) for a in range(NX) for b in range(4) for c in range(2)][1:]
    offsets.sort(key=lambda o: -(min(o[0], NX - o[0]) + min(o[1], 4 - o[1])))
    my_x, my_y, my_c = me // 8, lax.rem(me // 2, 4), lax.rem(me, 2)
    turn_of = 1 - 2 * my_c

    def to_plane_far(src, dst, rows, k, cols):
        for a, b, c in offsets:
            peer = (
                lax.rem(my_x + turn_of * a + NX, NX) * 8
                + lax.rem(my_y + turn_of * b + 4, 4) * 2
                + lax.rem(my_c + c, 2)
            )
            pltpu.make_async_remote_copy(
                src_ref=src.at[pl.ds(pl.multiple_of(peer * rows, rows), rows), 0:cols],
                dst_ref=dst.at[pl.ds(pl.multiple_of(me * rows, rows), rows)],
                send_sem=px.at[2 * k],
                recv_sem=px.at[2 * k + 1],
                device_id=(peer, z),
                device_id_type=MESH,
            ).start()

    def to_plane(src, by_peer, dst, rows, k):
        def body(i, c):
            half = (i + 1) // 2
            p = half + (1 - lax.rem(i, 2)) * (E - 2 * half)
            peer = lax.rem(me + p, E)
            if by_peer:
                piece = src.at[pl.ds(pl.multiple_of(peer * rows, rows), rows)]
            else:
                piece = src
            pltpu.make_async_remote_copy(
                src_ref=piece,
                dst_ref=dst.at[pl.ds(pl.multiple_of(me * rows, rows), rows)],
                send_sem=px.at[2 * k],
                recv_sem=px.at[2 * k + 1],
                device_id=(peer, z),
                device_id_type=MESH,
            ).start()
            return c

        lax.fori_loop(1, E, body, 0)

    def to_line(src, dst, rows, k):
        def body(p, c):
            pltpu.make_async_remote_copy(
                src_ref=src,
                dst_ref=dst.at[pl.ds(pl.multiple_of(z * rows, rows), rows)],
                send_sem=px.at[2 * k],
                recv_sem=px.at[2 * k + 1],
                device_id=(me, lax.rem(z + p, NZ)),
                device_id_type=MESH,
            ).start()
            return c

        lax.fori_loop(1, NZ, body, 0)

    def own_block(src, by_peer, dst, at, rows):
        here = pl.ds(pl.multiple_of(at * rows, rows), rows)
        dst[here, :] = src[here, :] if by_peer else src[...]

    def received(dst, rows, peers, k):
        wait_bytes(dst.at[pl.ds(0, (peers - 1) * rows)], px.at[2 * k + 1])

    def sent(dst, rows, peers, k):
        wait_bytes(dst.at[pl.ds(0, (peers - 1) * rows)], px.at[2 * k])

    experts = iota((E, T), 0)
    small[0].wait()
    member = (topT[0:1, :] == experts) | (topT[1:2, :] == experts)
    earlier = hot(iota((T, T), 0) < iota((T, T), 1))
    before = dot(hot(member), earlier)
    code = jnp.where(member, before, -1.0).astype(BF16)
    spread = hot(iota((S, E), 0) // MAIN == iota((S, E), 1))
    code_rows = dot(spread, code)
    place = lax.rem(iota((S, T), 0), MAIN)
    sel[...] = hot(code_rows == place.astype(F32))
    is_rest = code_rows == (lax.rem(place, REST) + MAIN).astype(F32)
    for q in range(SPLIT):
        selr[pl.ds(q * S, S), :] = hot(is_rest & (place // REST == q))

    RB = min(S, 128)

    def pack_rows(src, dst):
        def body(i, c):
            rows = pl.ds(pl.multiple_of(i * RB, RB), RB)
            dst[rows, 0:D] = dot(sel[rows, :], src[...]).astype(BF16)
            acc = jnp.zeros((RB, QD), F32)
            for q in range(SPLIT):
                pick = selr[pl.ds(pl.multiple_of(q * S + i * RB, RB), RB), :]
                acc += dot(pick, src[:, q * QD : (q + 1) * QD])
            dst[rows, D : D + QD] = acc.astype(BF16)
            return c

        lax.fori_loop(0, S // RB, body, 0)

    load_patches.wait()
    pack_rows(patches, send_x)
    pl.semaphore_wait(barrier, E + NZ - 2)
    to_plane_far(send_x, recv_x, MAIN, 0, D + QD)
    own_block(send_x, True, recv_x, me, MAIN)

    for load_small in small[1:]:
        load_small.wait()
    bias_pick = iota((E, E), 0) == iota((E, E), 1)
    bias_rows = jnp.sum(jnp.where(bias_pick, bias[...], 0.0), axis=1, keepdims=True)
    logits = dot_nt(rwT[...], patches[...]) + bias_rows
    noisy = logits + noiseT[...]
    top = jnp.max(noisy, axis=0, keepdims=True)
    powers = jnp.exp(noisy - top)
    probs = powers / jnp.sum(powers, axis=0, keepdims=True)
    thresh = thr[...] == experts
    base = jnp.sum(jnp.where(thresh, noisy, 0.0), axis=0, keepdims=True)
    zscore = logits - base
    probs_s[...] = probs
    z_s[...] = zscore
    prob_rows = dot(spread, probs.astype(BF16))
    gate_main = jnp.sum(prob_rows * sel[...].astype(F32), axis=1, keepdims=True)
    gate_rest = jnp.sum(jnp.where(is_rest, prob_rows, 0.0), axis=1, keepdims=True)
    lane_s = iota((S, 128), 1)
    place_s = lax.rem(iota((S, 128), 0), MAIN)
    gate_at = jnp.where(
        lane_s == place_s,
        gate_main,
        jnp.where((place_s < REST) & (lane_s == MAIN + place_s), gate_rest, 0.0),
    )
    by_expert = hot(iota((E, S), 1) // MAIN == iota((E, S), 0))
    gate_lists = dot(by_expert, gate_at.astype(BF16))
    for e in range(E):
        sgate[e] = gate_lists[e : e + 1, :]
    to_plane(sgate, True, rgate, 1, 8)
    own_block(sgate, True, rgate, me, 1)
    load_og.wait()
    pack_rows(og, send_g)
    to_plane_far(send_g, recv_g, MAIN, 1, D + QD)
    my_rows = pl.ds(pl.multiple_of(me * MAIN, MAIN), MAIN)
    recv_g[my_rows, :] = send_g[my_rows, 0 : D + QD]

    importance = jnp.sum(probs, axis=1, keepdims=True)
    load = jnp.sum(0.5 * (1.0 + lax.erf(zscore * inv_root_two)), axis=1, keepdims=True)
    row_id = iota((E, 128), 0)
    lane_id = iota((E, 128), 1)
    both = jnp.where(lane_id == row_id, importance, 0.0) + jnp.where(
        lane_id == row_id + E, load, 0.0
    )
    stat[...] = jnp.broadcast_to(jnp.sum(both, axis=0, keepdims=True), (8, 128))
    to_plane(stat, False, sr1, 8, 2)
    own_block(stat, False, sr1, me, 8)

    eye_t = hot(iota((T, T), 0) == iota((T, T), 1))
    selT[...] = dot_nt(eye_t, sel[...]).astype(BF16)
    for q in range(SPLIT):
        selrT[pl.ds(q * T, T), :] = dot_nt(eye_t, selr[pl.ds(q * S, S), :]).astype(BF16)
    for q in range(SPLIT):
        r = iota((R, S), 0)
        picks[pl.ds(q * R, R), :] = hot(
            iota((R, S), 1) == (r // REST) * MAIN + q * REST + lax.rem(r, REST)
        )
    load_in.wait()
    load_out.wait()

    def turn(i, c):
        cols = pl.ds(pl.multiple_of(i * 256, 256), 256)
        w_inT[cols, :] = w_in[:, cols].T
        return c

    lax.fori_loop(0, F // 256, turn, 0)

    def unpack_pick(q):
        return picks[pl.ds(q * R, R), :]

    def pack_pick(q):
        r = iota((S, R), 1)
        return hot(iota((S, R), 0) == (r // REST) * MAIN + q * REST + lax.rem(r, REST))

    def unpack(src, dst):
        dst[0:S, :] = src[:, 0:D]
        for q in range(SPLIT):
            dst[S:ROWS, q * QD : (q + 1) * QD] = dot(
                unpack_pick(q), src[:, D : D + QD]
            ).astype(BF16)

    def chunk_a(c, carry):
        rows = pl.ds(pl.multiple_of(c * FC, FC), FC)
        hidden = dot_nt(w_inT[rows, :], X[...])
        square = hidden * hidden
        t = jnp.tanh(gelu_k * (hidden + 0.044715 * (square * hidden)))
        cdf = 0.5 * (1.0 + t)
        AT[rows, :] = (hidden * cdf).astype(BF16)
        slope[rows, :] = cdf + hidden * (0.5 * (1.0 - t * t)) * (
            gelu_k * (1.0 + (3.0 * 0.044715) * square)
        )
        return carry

    received(recv_x, MAIN, E, 0)
    unpack(recv_x, X)
    lax.fori_loop(0, NZ, chunk_a, 0)
    received(rgate, 1, E, 8)
    gate_lists = jnp.concatenate([rgate[e] for e in range(E)], axis=0).astype(BF16)
    main_lists = dot(hot(iota((S, E), 0) // MAIN == iota((S, E), 1)), gate_lists)
    rest_lists = dot(hot(iota((R, E), 0) // REST == iota((R, E), 1)), gate_lists)
    main_here = iota((S, 128), 1) == lax.rem(iota((S, 128), 0), MAIN)
    rest_here = iota((R, 128), 1) == MAIN + lax.rem(iota((R, 128), 0), REST)
    gate_main = jnp.sum(jnp.where(main_here, main_lists, 0.0), axis=1, keepdims=True)
    gate_rest = jnp.sum(jnp.where(rest_here, rest_lists, 0.0), axis=1, keepdims=True)
    first_lane = hot(iota((8, 128), 1) == 0)
    growr[:, 0:S] = dot_nt(first_lane, jnp.broadcast_to(gate_main, (S, 128)).astype(BF16))
    growr[:, S:ROWS] = dot_nt(first_lane, jnp.broadcast_to(gate_rest, (R, 128)).astype(BF16))
    gt[...] = jnp.zeros_like(gt)
    received(recv_g, MAIN, E, 1)
    for q in range(SPLIT):
        G[S:ROWS, q * QD : (q + 1) * QD] = dot(
            unpack_pick(q), recv_g[:, D : D + QD]
        ).astype(BF16)
    SG[0:S, :] = (gate_main * recv_g[:, 0:D].astype(F32)).astype(BF16)
    SG[S:ROWS, :] = (gate_rest * G[S:ROWS, :].astype(F32)).astype(BF16)

    def chunk_b(c):
        rows = pl.ds(pl.multiple_of(c * FC, FC), FC)
        back = dot_nt(w_out[rows, :], G[...])
        HT[rows, :] = ((growr[0:1, :] * back) * slope[rows, :]).astype(BF16)
        gt[0:1, :] += jnp.sum(back * AT[rows, :].astype(F32), axis=0, keepdims=True)

    def at_offset(o):
        return lax.rem(z + o + 2 * NZ, NZ)

    def line_copy(src, buf, s, h, to, k):
        i = s * NSUB + h
        return pltpu.make_async_remote_copy(
            src_ref=src,
            dst_ref=buf.at[pl.ds(pl.multiple_of(i * SUB, SUB), SUB)],
            send_sem=ring_sem.at[2 * k, i],
            recv_sem=ring_sem.at[2 * k + 1, i],
            device_id=(me, to),
            device_id_type=MESH,
        )

    cw0, ccw0 = w_inT.at[pl.ds(0, FC)], w_inT.at[pl.ds(FC, FC)]
    rbT = w_inT.at[pl.ds(F // 2, D), 0:ROWS]
    send_b = send_g
    ways = ((AT, SG, cw0, cw, -1), (HT, X, ccw0, ccw, 1))

    def product(s, k):
        left, right, _, _, sign = ways[k]
        rows = pl.ds(pl.multiple_of(at_offset(sign * (1 + s)) * FC, FC), FC)
        own[k * FC : (k + 1) * FC, :] = dot(left[rows, :], right[...])

    def own_piece(k, h):
        return own[pl.ds(pl.multiple_of(k * FC + h * SUB, SUB), SUB), :]

    def ring_first(k):
        _, _, buf0, buf, sign = ways[k]

        def body(h, c):
            place_at = buf0.at[pl.ds(pl.multiple_of(h * SUB, SUB), SUB)]
            place_at[...] = own_piece(k, h).astype(BF16)
            line_copy(place_at, buf, 0, h, at_offset(-sign), k).start()
            return c

        lax.fori_loop(0, NSUB, body, 0)

    def ring_step(s):
        def body(h, c):
            for k, (_, _, _, buf, sign) in enumerate(ways):
                i = (s - 1) * NSUB + h
                place_at = buf.at[pl.ds(pl.multiple_of(i * SUB, SUB), SUB)]
                wait_bytes(place_at, ring_sem.at[2 * k + 1, i])
                place_at[...] = (own_piece(k, h) + place_at[...].astype(F32)).astype(BF16)
                line_copy(place_at, buf, s, h, at_offset(-sign), k).start()
            return c

        lax.fori_loop(0, NSUB, body, 0)

    whole_outs = [
        pltpu.make_async_copy(a, b, osem.at[i])
        for i, (a, b) in enumerate(((pg, pg_hbm), (rb, rb_hbm), (rgT, rgT_hbm)))
    ]

    def piece_out(k, h):
        src, dst = ((wo, wo_hbm), (wiT, wiT_hbm))[k]
        here = pl.ds(pl.multiple_of(h * SUB, SUB), SUB)
        return pltpu.make_async_copy(src.at[here], dst.at[here], osem.at[3 + k * NSUB + h])

    def ring_end():
        outs = (wo, wiT)

        def body(h, c):
            for k, (_, _, _, buf, _) in enumerate(ways):
                i = (NZ - 2) * NSUB + h
                last = buf.at[pl.ds(pl.multiple_of(i * SUB, SUB), SUB)]
                wait_bytes(last, ring_sem.at[2 * k + 1, i])
                here = pl.ds(pl.multiple_of(h * SUB, SUB), SUB)
                outs[k][here, :] = (own_piece(k, h) + last[...].astype(F32)).astype(BF16)
                piece_out(k, h).start()
            return c

        lax.fori_loop(0, NSUB, body, 0)

    def backs(lo, hi):
        def body(i, c):
            chunk_b(at_offset(i))
            return c

        lax.fori_loop(lo, hi, body, 0)

    def stats_on():
        received(sr1, 8, E, 2)
        total = sr1[0:8, :]
        for j in range(1, E):
            total += sr1[j * 8 : (j + 1) * 8, :]
        ss2[...] = total
        to_line(ss2, sr2, 8, 3)
        own_block(ss2, False, sr2, z, 8)

    def rows_home():
        def body(i, c):
            rows = pl.ds(pl.multiple_of(i * QD, QD), QD)
            rbT[rows, :] = dot(w_in[rows, :], HT[...]).astype(BF16)
            return c

        lax.fori_loop(0, SPLIT, body, 0)
        sent(recv_g, MAIN, E, 1)
        eye_s = hot(iota((S, S), 0) == iota((S, S), 1))
        rest = jnp.zeros((S, QD), F32)
        for q in range(SPLIT):
            cols = slice(q * QD, (q + 1) * QD)
            send_b[:, cols] = dot_nt(eye_s, rbT[cols, 0:S]).astype(BF16)
            rest += dot_nt(pack_pick(q), rbT[cols, S:ROWS])
        send_b[:, D : D + QD] = rest.astype(BF16)
        terms = jnp.broadcast_to(gt[0:1, :], (128, ROWS)).astype(BF16)
        r = iota((S, R), 1)
        s_ = iota((S, R), 0)
        any_pick = hot((s_ // MAIN == r // REST) & (lax.rem(s_, REST) == lax.rem(r, REST)))
        term_main = dot_nt(eye_s, terms[:, 0:S])
        term_rest = dot_nt(any_pick, terms[:, S:ROWS])
        send_b[:, D + QD : D + QD + 128] = jnp.where(
            iota((S, 128), 1) < 64, term_main, term_rest
        ).astype(BF16)
        to_plane_far(send_b, recv_b, MAIN, 4, D + QD + 128)
        own_block(send_b, True, recv_b, me, MAIN)

    def spread_grad(v):
        average = jnp.mean(v, axis=0, keepdims=True)
        dev = jnp.mean((v - average) ** 2, axis=0, keepdims=True)
        return (2.0 * (v - average) - 2.0 * dev / average) / (E * average * average)

    def at_home():
        received(sr2, 8, NZ, 3)
        received(recv_b, MAIN, E, 4)
        total = sr2[0:8, :]
        for j in range(1, NZ):
            total += sr2[j * 8 : (j + 1) * 8, :]
        row = jnp.broadcast_to(total[0:1, :], (E, 128))
        imp = jnp.sum(jnp.where(lane_id == row_id, row, 0.0), axis=1, keepdims=True)
        ld = jnp.sum(jnp.where(lane_id == row_id + E, row, 0.0), axis=1, keepdims=True)
        imp_coef = TOTAL * spread_grad(imp)
        load_coef = TOTAL * spread_grad(ld)
        probs = probs_s[...]
        zscore = z_s[...]
        tile = recv_b[:, D + QD : D + QD + 128].astype(F32)
        weighted = sel[...].astype(F32) * tile[:, 0:1] + selr[0:S, :].astype(F32) * tile[:, 64:65]
        gather = hot(iota((E, S), 1) // MAIN == iota((E, S), 0))
        score = dot(gather, weighted.astype(BF16)) + imp_coef
        noisy_grad = probs * (score - jnp.sum(probs * score, axis=0, keepdims=True))
        z_grad = load_coef * inv_root_tau * jnp.exp(-0.5 * zscore * zscore)
        thresh = thr[...] == iota((E, T), 0)
        logit_grad = (
            noisy_grad
            + z_grad
            - jnp.where(thresh, jnp.sum(z_grad, axis=0, keepdims=True), 0.0)
        )
        low = logit_grad.astype(BF16)
        llT_s[...] = low
        weight_part = dot(low, patches[...])
        bias_col = jnp.sum(logit_grad, axis=1, keepdims=True)
        bias_row = jnp.sum(jnp.where(lane_id == row_id, bias_col, 0.0), axis=0, keepdims=True)
        bias_tile = jnp.broadcast_to(bias_row, (8, 128))
        tiles = D // 128
        for p in range(E):
            a, b = p // tiles, p % tiles
            ws1[p * 16 : p * 16 + 8, :] = weight_part[a * 8 : a * 8 + 8, b * 128 : b * 128 + 128]
            ws1[p * 16 + 8 : p * 16 + 16, :] = bias_tile
        to_plane(ws1, True, wr1, 16, 5)
        own_block(ws1, True, wr1, me, 16)
        low_rows = dot_nt(eye_t, llT_s[...]).astype(BF16)
        for q in range(SPLIT):
            cols = slice(q * QD, (q + 1) * QD)
            out = dot(selT[...], recv_b[:, cols])
            out += dot(selrT[pl.ds(q * T, T), :], recv_b[:, D : D + QD])
            out += dot(low_rows, rwT[:, cols])
            pg[:, cols] = out.astype(BF16)
        whole_outs[0].start()

    def reduce_plane():
        received(wr1, 16, E, 5)
        total = wr1[0:16, :]
        for j in range(1, E):
            total += wr1[j * 16 : (j + 1) * 16, :]
        ws2[...] = total
        to_line(ws2, wr2, 16, 6)
        own_block(ws2, False, wr2, z, 16)

    def reduce_line():
        received(wr2, 16, NZ, 6)
        total = wr2[0:16, :]
        for j in range(1, NZ):
            total += wr2[j * 16 : (j + 1) * 16, :]
        rb[...] = total[8:16, :]
        whole_outs[1].start()
        ws3[...] = total[0:8, :]
        to_plane(ws3, False, wr3, 8, 7)
        own_block(ws3, False, wr3, me, 8)

    def spread_total():
        received(wr3, 8, E, 7)
        tiles = D // 128
        for p in range(E):
            a, b = p // tiles, p % tiles
            rgT[a * 8 : a * 8 + 8, b * 128 : b * 128 + 128] = wr3[p * 8 : p * 8 + 8, :]
        whole_outs[2].start()

    works = (rows_home, at_home, reduce_plane, reduce_line, spread_total)
    gaps = dict(zip((2, 4, 5, 6), works)) if NZ == 8 else {}
    product(0, 0)
    ring_first(0)
    G[0:S, :] = recv_g[:, 0:D]
    backs(1, 2)
    product(0, 1)
    ring_first(1)
    half = NZ // 2
    for s in range(NZ - 1):
        if s > 0:
            ring_step(s)
        if s == 0:
            backs(2, half + 1)
        if s == 1 or NZ == 2:
            backs(half + 1, NZ + 1)
        product(s + 1, 0)
        product(s + 1, 1)
        if s == 1 or NZ == 2:
            stats_on()
        if s in gaps:
            gaps[s]()
    ring_end()
    for work in works[len(gaps):]:
        work()

    sent(recv_x, MAIN, E, 0)
    sent(sr1, 8, E, 2)
    sent(sr2, 8, NZ, 3)
    sent(recv_b, MAIN, E, 4)
    sent(wr1, 16, E, 5)
    sent(wr2, 16, NZ, 6)
    sent(wr3, 8, E, 7)
    sent(rgate, 1, E, 8)

    def drain(i, c):
        for k, way in enumerate(ways):
            wait_bytes(way[2].at[pl.ds(0, SUB)], ring_sem.at[2 * k, i])
        return c

    lax.fori_loop(0, (NZ - 1) * NSUB, drain, 0)

    for copy in whole_outs:
        copy.wait()

    def written(h, c):
        piece_out(0, h).wait()
        piece_out(1, h).wait()
        return c

    lax.fori_loop(0, NSUB, written, 0)


def finish(pg, wiT, wo, rgT, rb, pg_out, wi_out, wo_out, rgT_out, rb_out):
    pg_out[...] = pg[...]
    wi_out[...] = wiT[...].T
    wo_out[...] = wo[...]
    rgT_out[...] = rgT[...]
    rb_out[...] = rb[0:1, 0 : rb_out.shape[1]]


def on_device(
    patches, router_weight, router_bias, noise, top_experts, threshold_expert, w_in, w_out, out_grad
):
    T, D = patches.shape
    E = router_weight.shape[1]
    NZ = lax.axis_size("dp")
    F = w_in.shape[2]
    FC = F // NZ
    S = E * MAIN
    ROWS = S + E * REST
    QD = D // SPLIT
    WX = D + QD
    WG = WX + 128
    VMEM = pltpu.VMEM
    whole = pl.BlockSpec(memory_space=pltpu.VMEM)
    far = pl.BlockSpec(memory_space=pltpu.HBM)
    pg, wiT, wo, rgT, rb = pl.pallas_call(
        functools.partial(kernel, E, NZ, float(T * E * NZ)),
        out_shape=(
            jax.ShapeDtypeStruct((T, D), BF16),
            jax.ShapeDtypeStruct((FC, D), BF16),
            jax.ShapeDtypeStruct((FC, D), BF16),
            jax.ShapeDtypeStruct((E, D), F32),
            jax.ShapeDtypeStruct((8, 128), F32),
        ),
        in_specs=[far] * 9,
        out_specs=(far,) * 5,
        scratch_shapes=[
            VMEM((T, D), BF16), VMEM((FC, D), BF16), VMEM((FC, D), BF16), VMEM((E, D), F32),
            VMEM((8, 128), F32), pltpu.SemaphoreType.DMA((3 + 2 * NSUB,)),
            VMEM((E, 1, 128), F32), VMEM((E, 1, 128), F32),
            VMEM((E, D), BF16), VMEM((1, E), F32), VMEM((E, T), F32),
            VMEM((2, T), jnp.int32), VMEM((1, T), jnp.int32),
            VMEM((T, D), BF16), VMEM((T, D), BF16),
            VMEM((D, F), BF16), VMEM((F, D), BF16), VMEM((F, D), BF16),
            VMEM((SPLIT * E * REST, S), BF16), VMEM((F, ROWS), F32), VMEM((2 * FC, D), F32),
            VMEM((S, T), BF16), VMEM((SPLIT * S, T), BF16),
            VMEM((T, S), BF16), VMEM((SPLIT * T, S), BF16),
            VMEM((S, WX), BF16), VMEM((S, WG), BF16), VMEM((S, WX), BF16), VMEM((S, WX), BF16),
            VMEM((S, WG), BF16),
            VMEM((ROWS, D), BF16), VMEM((ROWS, D), BF16), VMEM((ROWS, D), BF16),
            VMEM((F, ROWS), BF16), VMEM((F, ROWS), BF16),
            VMEM((8, ROWS), F32), VMEM((8, ROWS), F32),
            VMEM(((NZ - 1) * FC, D), BF16),
            VMEM(((NZ - 1) * FC, D), BF16),
            VMEM((E, T), F32), VMEM((E, T), F32), VMEM((E, T), BF16),
            VMEM((8, 128), F32), VMEM((E * 8, 128), F32),
            VMEM((8, 128), F32), VMEM((NZ * 8, 128), F32),
            VMEM((E * 16, 128), F32), VMEM((E * 16, 128), F32),
            VMEM((16, 128), F32), VMEM((NZ * 16, 128), F32),
            VMEM((8, 128), F32), VMEM((E * 8, 128), F32),
            pltpu.SemaphoreType.DMA((9,)),
            pltpu.SemaphoreType.DMA((18,)),
            pltpu.SemaphoreType.DMA((4, (NZ - 1) * NSUB)),
        ],
        compiler_params=pltpu.CompilerParams(
            collective_id=0, has_side_effects=True, vmem_limit_bytes=58 * 1024 * 1024
        ),
        name="moe_back",
    )(
        patches,
        router_weight.T,
        router_bias.reshape(1, E),
        noise.T,
        top_experts.T,
        threshold_expert.reshape(1, T),
        out_grad,
        w_in[0],
        w_out[0],
    )
    pg, wi, wo, rgT, rb = pl.pallas_call(
        finish,
        out_shape=(
            jax.ShapeDtypeStruct((T, D), BF16),
            jax.ShapeDtypeStruct((D, FC), BF16),
            jax.ShapeDtypeStruct((FC, D), BF16),
            jax.ShapeDtypeStruct((E, D), F32),
            jax.ShapeDtypeStruct((1, E), F32),
        ),
        in_specs=[whole] * 5,
        out_specs=(whole,) * 5,
        compiler_params=pltpu.CompilerParams(vmem_limit_bytes=62 * 1024 * 1024),
        name="moe_back_out",
    )(pg, wiT, wo, rgT, rb)
    return (pg, wi[None], wo[None], rgT.T, rb[0])


def solution(mesh):
    both = ("expert", "dp")
    in_specs = (
        P(both, None), P(), P(), P(both, None), P(both, None), P(both),
        P("expert", None, None), P("expert", None, None), P(both, None),
    )
    out_specs = (P(both, None), P("expert", None, "dp"), P("expert", "dp", None), P(), P())
    return jax.shard_map(
        on_device, mesh=mesh, in_specs=in_specs, out_specs=out_specs, check_vma=False
    )
```

```python
import functools
import math

import jax
import jax.numpy as jnp
from jax import lax
from jax.experimental import pallas as pl
from jax.experimental.pallas import tpu as pltpu
from jax.sharding import PartitionSpec as P

F32 = jnp.float32
BF16 = jnp.bfloat16
MESH = pl.DeviceIdType.MESH
MAIN = 16
REST = 4
SPLIT = 4
NSUB = 2
inv_root_two = 0.7071067811865476
inv_root_tau = 0.3989422804014327
gelu_k = math.sqrt(2.0 / math.pi)


def dot(a, b):
    return jnp.dot(a, b, preferred_element_type=F32)


def dot_nt(a, b):
    return lax.dot_general(a, b, (((1,), (1,)), ((), ())), preferred_element_type=F32)


def iota(shape, dim):
    return lax.broadcasted_iota(jnp.int32, shape, dim)


def hot(mask):
    return jnp.where(mask, 1.0, 0.0).astype(BF16)


def wait_bytes(ref, sem):
    pltpu.make_async_copy(ref, ref, sem).wait()


def kernel(
    E, NZ, TOTAL,
    patches_hbm, rwT_hbm, bias_hbm, noiseT_hbm, topT_hbm, thr_hbm, og_hbm, w_in_hbm, w_out_hbm,
    pg_hbm, wiT_hbm, wo_hbm, rgT_hbm, rb_hbm,
    pg, wiT, wo, rgT, rb, osem, sgate, rgate, rwT, bias, noiseT, topT, thr, patches, og, w_in, w_out, w_inT, picks, slope, own, sel, selr, selT, selrT, send_x, send_g, recv_x, recv_g,
    recv_b, X, G, SG, AT, HT, growr, gt, cw, ccw,
    probs_s, z_s, llT_s, stat, sr1, ss2, sr2, ws1, wr1, ws2, wr2, ws3, wr3, wsem, px, ring_sem,
):
    T, D = patches.shape
    F = w_out.shape[0]
    FC = F // NZ
    SUB = FC // NSUB
    QD = D // SPLIT
    S = E * MAIN
    R = E * REST
    ROWS = S + R
    me = lax.axis_index("expert")
    z = lax.axis_index("dp")

    load_patches = pltpu.make_async_copy(patches_hbm, patches, wsem.at[2])
    load_og = pltpu.make_async_copy(og_hbm, og, wsem.at[3])
    small = [
        pltpu.make_async_copy(a, b, wsem.at[4 + i])
        for i, (a, b) in enumerate(
            ((topT_hbm, topT), (rwT_hbm, rwT), (bias_hbm, bias), (noiseT_hbm, noiseT), (thr_hbm, thr))
        )
    ]
    small[0].start()
    load_patches.start()
    for load_small in small[1:]:
        load_small.start()
    load_og.start()
    load_in = pltpu.make_async_copy(w_in_hbm, w_in, wsem.at[0])
    load_out = pltpu.make_async_copy(w_out_hbm, w_out, wsem.at[1])
    load_in.start()
    load_out.start()

    barrier = pltpu.get_barrier_semaphore()

    def greet_plane(p, c):
        pl.semaphore_signal(
            barrier, inc=1, device_id=(lax.rem(me + p, E), z), device_id_type=MESH
        )
        return c

    def greet_line(p, c):
        pl.semaphore_signal(
            barrier, inc=1, device_id=(me, lax.rem(z + p, NZ)), device_id_type=MESH
        )
        return c

    lax.fori_loop(1, E, greet_plane, 0)
    lax.fori_loop(1, NZ, greet_line, 0)

    NX = E // 8
    offsets = [(a, b, c) for a in range(NX) for b in range(4) for c in range(2)][1:]
    offsets.sort(key=lambda o: -(min(o[0], NX - o[0]) + min(o[1], 4 - o[1])))
    my_x, my_y, my_c = me // 8, lax.rem(me // 2, 4), lax.rem(me, 2)
    turn_of = 1 - 2 * my_c

    def to_plane_far(src, dst, rows, k, cols):
        for a, b, c in offsets:
            peer = (
                lax.rem(my_x + turn_of * a + NX, NX) * 8
                + lax.rem(my_y + turn_of * b + 4, 4) * 2
                + lax.rem(my_c + c, 2)
            )
            pltpu.make_async_remote_copy(
                src_ref=src.at[pl.ds(pl.multiple_of(peer * rows, rows), rows), 0:cols],
                dst_ref=dst.at[pl.ds(pl.multiple_of(me * rows, rows), rows)],
                send_sem=px.at[2 * k],
                recv_sem=px.at[2 * k + 1],
                device_id=(peer, z),
                device_id_type=MESH,
            ).start()

    def to_plane(src, by_peer, dst, rows, k):
        def body(i, c):
            half = (i + 1) // 2
            p = half + (1 - lax.rem(i, 2)) * (E - 2 * half)
            peer = lax.rem(me + p, E)
            if by_peer:
                piece = src.at[pl.ds(pl.multiple_of(peer * rows, rows), rows)]
            else:
                piece = src
            pltpu.make_async_remote_copy(
                src_ref=piece,
                dst_ref=dst.at[pl.ds(pl.multiple_of(me * rows, rows), rows)],
                send_sem=px.at[2 * k],
                recv_sem=px.at[2 * k + 1],
                device_id=(peer, z),
                device_id_type=MESH,
            ).start()
            return c

        lax.fori_loop(1, E, body, 0)

    def to_line(src, dst, rows, k):
        def body(p, c):
            pltpu.make_async_remote_copy(
                src_ref=src,
                dst_ref=dst.at[pl.ds(pl.multiple_of(z * rows, rows), rows)],
                send_sem=px.at[2 * k],
                recv_sem=px.at[2 * k + 1],
                device_id=(me, lax.rem(z + p, NZ)),
                device_id_type=MESH,
            ).start()
            return c

        lax.fori_loop(1, NZ, body, 0)

    def own_block(src, by_peer, dst, at, rows):
        here = pl.ds(pl.multiple_of(at * rows, rows), rows)
        dst[here, :] = src[here, :] if by_peer else src[...]

    def received(dst, rows, peers, k):
        wait_bytes(dst.at[pl.ds(0, (peers - 1) * rows)], px.at[2 * k + 1])

    def sent(dst, rows, peers, k):
        wait_bytes(dst.at[pl.ds(0, (peers - 1) * rows)], px.at[2 * k])

    experts = iota((E, T), 0)
    small[0].wait()
    member = (topT[0:1, :] == experts) | (topT[1:2, :] == experts)
    earlier = hot(iota((T, T), 0) < iota((T, T), 1))
    before = dot(hot(member), earlier)
    code = jnp.where(member, before, -1.0).astype(BF16)
    spread = hot(iota((S, E), 0) // MAIN == iota((S, E), 1))
    code_rows = dot(spread, code)
    place = lax.rem(iota((S, T), 0), MAIN)
    sel[...] = hot(code_rows == place.astype(F32))
    is_rest = code_rows == (lax.rem(place, REST) + MAIN).astype(F32)
    for q in range(SPLIT):
        selr[pl.ds(q * S, S), :] = hot(is_rest & (place // REST == q))

    RB = min(S, 128)

    def pack_rows(src, dst):
        def body(i, c):
            rows = pl.ds(pl.multiple_of(i * RB, RB), RB)
            dst[rows, 0:D] = dot(sel[rows, :], src[...]).astype(BF16)
            acc = jnp.zeros((RB, QD), F32)
            for q in range(SPLIT):
                pick = selr[pl.ds(pl.multiple_of(q * S + i * RB, RB), RB), :]
                acc += dot(pick, src[:, q * QD : (q + 1) * QD])
            dst[rows, D : D + QD] = acc.astype(BF16)
            return c

        lax.fori_loop(0, S // RB, body, 0)

    load_patches.wait()
    pack_rows(patches, send_x)
    pl.semaphore_wait(barrier, E + NZ - 2)
    to_plane_far(send_x, recv_x, MAIN, 0, D + QD)
    own_block(send_x, True, recv_x, me, MAIN)

    for load_small in small[1:]:
        load_small.wait()
    bias_pick = iota((E, E), 0) == iota((E, E), 1)
    bias_rows = jnp.sum(jnp.where(bias_pick, bias[...], 0.0), axis=1, keepdims=True)
    logits = dot_nt(rwT[...], patches[...]) + bias_rows
    noisy = logits + noiseT[...]
    top = jnp.max(noisy, axis=0, keepdims=True)
    powers = jnp.exp(noisy - top)
    probs = powers / jnp.sum(powers, axis=0, keepdims=True)
    thresh = thr[...] == experts
    base = jnp.sum(jnp.where(thresh, noisy, 0.0), axis=0, keepdims=True)
    zscore = logits - base
    probs_s[...] = probs
    z_s[...] = zscore
    prob_rows = dot(spread, probs.astype(BF16))
    gate_main = jnp.sum(prob_rows * sel[...].astype(F32), axis=1, keepdims=True)
    gate_rest = jnp.sum(jnp.where(is_rest, prob_rows, 0.0), axis=1, keepdims=True)
    lane_s = iota((S, 128), 1)
    place_s = lax.rem(iota((S, 128), 0), MAIN)
    gate_at = jnp.where(
        lane_s == place_s,
        gate_main,
        jnp.where((place_s < REST) & (lane_s == MAIN + place_s), gate_rest, 0.0),
    )
    by_expert = hot(iota((E, S), 1) // MAIN == iota((E, S), 0))
    gate_lists = dot(by_expert, gate_at.astype(BF16))
    for e in range(E):
        sgate[e] = gate_lists[e : e + 1, :]
    to_plane(sgate, True, rgate, 1, 8)
    own_block(sgate, True, rgate, me, 1)
    load_og.wait()
    pack_rows(og, send_g)
    to_plane_far(send_g, recv_g, MAIN, 1, D + QD)
    my_rows = pl.ds(pl.multiple_of(me * MAIN, MAIN), MAIN)
    recv_g[my_rows, :] = send_g[my_rows, 0 : D + QD]

    importance = jnp.sum(probs, axis=1, keepdims=True)
    load = jnp.sum(0.5 * (1.0 + lax.erf(zscore * inv_root_two)), axis=1, keepdims=True)
    row_id = iota((E, 128), 0)
    lane_id = iota((E, 128), 1)
    both = jnp.where(lane_id == row_id, importance, 0.0) + jnp.where(
        lane_id == row_id + E, load, 0.0
    )
    stat[...] = jnp.broadcast_to(jnp.sum(both, axis=0, keepdims=True), (8, 128))
    to_plane(stat, False, sr1, 8, 2)
    own_block(stat, False, sr1, me, 8)

    eye_t = hot(iota((T, T), 0) == iota((T, T), 1))
    selT[...] = dot_nt(eye_t, sel[...]).astype(BF16)
    for q in range(SPLIT):
        selrT[pl.ds(q * T, T), :] = dot_nt(eye_t, selr[pl.ds(q * S, S), :]).astype(BF16)
    for q in range(SPLIT):
        r = iota((R, S), 0)
        picks[pl.ds(q * R, R), :] = hot(
            iota((R, S), 1) == (r // REST) * MAIN + q * REST + lax.rem(r, REST)
        )
    load_in.wait()
    load_out.wait()

    def turn(i, c):
        cols = pl.ds(pl.multiple_of(i * 256, 256), 256)
        w_inT[cols, :] = w_in[:, cols].T
        return c

    lax.fori_loop(0, F // 256, turn, 0)

    def unpack_pick(q):
        return picks[pl.ds(q * R, R), :]

    def pack_pick(q):
        r = iota((S, R), 1)
        return hot(iota((S, R), 0) == (r // REST) * MAIN + q * REST + lax.rem(r, REST))

    def unpack(src, dst):
        dst[0:S, :] = src[:, 0:D]
        for q in range(SPLIT):
            dst[S:ROWS, q * QD : (q + 1) * QD] = dot(
                unpack_pick(q), src[:, D : D + QD]
            ).astype(BF16)

    def chunk_a(c, carry):
        rows = pl.ds(pl.multiple_of(c * FC, FC), FC)
        hidden = dot_nt(w_inT[rows, :], X[...])
        square = hidden * hidden
        t = jnp.tanh(gelu_k * (hidden + 0.044715 * (square * hidden)))
        cdf = 0.5 * (1.0 + t)
        AT[rows, :] = (hidden * cdf).astype(BF16)
        slope[rows, :] = cdf + hidden * (0.5 * (1.0 - t * t)) * (
            gelu_k * (1.0 + (3.0 * 0.044715) * square)
        )
        return carry

    received(recv_x, MAIN, E, 0)
    unpack(recv_x, X)
    lax.fori_loop(0, NZ, chunk_a, 0)
    received(rgate, 1, E, 8)
    gate_lists = jnp.concatenate([rgate[e] for e in range(E)], axis=0).astype(BF16)
    main_lists = dot(hot(iota((S, E), 0) // MAIN == iota((S, E), 1)), gate_lists)
    rest_lists = dot(hot(iota((R, E), 0) // REST == iota((R, E), 1)), gate_lists)
    main_here = iota((S, 128), 1) == lax.rem(iota((S, 128), 0), MAIN)
    rest_here = iota((R, 128), 1) == MAIN + lax.rem(iota((R, 128), 0), REST)
    gate_main = jnp.sum(jnp.where(main_here, main_lists, 0.0), axis=1, keepdims=True)
    gate_rest = jnp.sum(jnp.where(rest_here, rest_lists, 0.0), axis=1, keepdims=True)
    first_lane = hot(iota((8, 128), 1) == 0)
    growr[:, 0:S] = dot_nt(first_lane, jnp.broadcast_to(gate_main, (S, 128)).astype(BF16))
    growr[:, S:ROWS] = dot_nt(first_lane, jnp.broadcast_to(gate_rest, (R, 128)).astype(BF16))
    gt[...] = jnp.zeros_like(gt)
    received(recv_g, MAIN, E, 1)
    for q in range(SPLIT):
        G[S:ROWS, q * QD : (q + 1) * QD] = dot(
            unpack_pick(q), recv_g[:, D : D + QD]
        ).astype(BF16)
    SG[0:S, :] = (gate_main * recv_g[:, 0:D].astype(F32)).astype(BF16)
    SG[S:ROWS, :] = (gate_rest * G[S:ROWS, :].astype(F32)).astype(BF16)

    def chunk_b(c, first=False):
        rows = pl.ds(pl.multiple_of(c * FC, FC), FC)
        if first:
            back = jnp.concatenate(
                [dot_nt(w_out[rows, :], recv_g[:, 0:D]), dot_nt(w_out[rows, :], G[S:ROWS, :])], axis=1
            )
        else:
            back = dot_nt(w_out[rows, :], G[...])
        HT[rows, :] = ((growr[0:1, :] * back) * slope[rows, :]).astype(BF16)
        gt[0:1, :] += jnp.sum(back * AT[rows, :].astype(F32), axis=0, keepdims=True)

    def at_offset(o):
        return lax.rem(z + o + 2 * NZ, NZ)

    def line_copy(src, buf, s, h, to, k):
        i = s * NSUB + h
        return pltpu.make_async_remote_copy(
            src_ref=src,
            dst_ref=buf.at[pl.ds(pl.multiple_of(i * SUB, SUB), SUB)],
            send_sem=ring_sem.at[2 * k, i],
            recv_sem=ring_sem.at[2 * k + 1, i],
            device_id=(me, to),
            device_id_type=MESH,
        )

    cw0, ccw0 = w_inT.at[pl.ds(0, FC)], w_inT.at[pl.ds(FC, FC)]
    rbT = w_inT.at[pl.ds(F // 2, D), 0:ROWS]
    send_b = send_g
    ways = ((AT, SG, cw0, cw, -1), (HT, X, ccw0, ccw, 1))

    def product(s, k):
        left, right, _, _, sign = ways[k]
        rows = pl.ds(pl.multiple_of(at_offset(sign * (1 + s)) * FC, FC), FC)
        own[k * FC : (k + 1) * FC, :] = dot(left[rows, :], right[...])

    def own_piece(k, h):
        return own[pl.ds(pl.multiple_of(k * FC + h * SUB, SUB), SUB), :]

    def ring_first(k):
        _, _, buf0, buf, sign = ways[k]

        def body(h, c):
            place_at = buf0.at[pl.ds(pl.multiple_of(h * SUB, SUB), SUB)]
            place_at[...] = own_piece(k, h).astype(BF16)
            line_copy(place_at, buf, 0, h, at_offset(-sign), k).start()
            return c

        lax.fori_loop(0, NSUB, body, 0)

    def ring_step(s):
        def body(h, c):
            for k, (_, _, _, buf, sign) in enumerate(ways):
                i = (s - 1) * NSUB + h
                place_at = buf.at[pl.ds(pl.multiple_of(i * SUB, SUB), SUB)]
                wait_bytes(place_at, ring_sem.at[2 * k + 1, i])
                place_at[...] = (own_piece(k, h) + place_at[...].astype(F32)).astype(BF16)
                line_copy(place_at, buf, s, h, at_offset(-sign), k).start()
            return c

        lax.fori_loop(0, NSUB, body, 0)

    whole_outs = [
        pltpu.make_async_copy(a, b, osem.at[i])
        for i, (a, b) in enumerate(((pg, pg_hbm), (rb, rb_hbm), (rgT, rgT_hbm)))
    ]

    def piece_out(k, h):
        src, dst = ((wo, wo_hbm), (wiT, wiT_hbm))[k]
        here = pl.ds(pl.multiple_of(h * SUB, SUB), SUB)
        return pltpu.make_async_copy(src.at[here], dst.at[here], osem.at[3 + k * NSUB + h])

    def ring_end(lo, hi):
        outs = (wo, wiT)

        def body(h, c):
            for k, (_, _, _, buf, _) in enumerate(ways):
                i = (NZ - 2) * NSUB + h
                last = buf.at[pl.ds(pl.multiple_of(i * SUB, SUB), SUB)]
                wait_bytes(last, ring_sem.at[2 * k + 1, i])
                here = pl.ds(pl.multiple_of(h * SUB, SUB), SUB)
                outs[k][here, :] = (own_piece(k, h) + last[...].astype(F32)).astype(BF16)
                piece_out(k, h).start()
            return c

        lax.fori_loop(lo, hi, body, 0)

    def backs(lo, hi):
        def body(i, c):
            chunk_b(at_offset(i))
            return c

        lax.fori_loop(lo, hi, body, 0)

    def stats_on():
        received(sr1, 8, E, 2)
        total = sr1[0:8, :]
        for j in range(1, E):
            total += sr1[j * 8 : (j + 1) * 8, :]
        ss2[...] = total
        to_line(ss2, sr2, 8, 3)
        own_block(ss2, False, sr2, z, 8)

    def rows_home():
        def body(i, c):
            rows = pl.ds(pl.multiple_of(i * QD, QD), QD)
            rbT[rows, :] = dot(w_in[rows, :], HT[...]).astype(BF16)
            return c

        lax.fori_loop(0, SPLIT, body, 0)
        sent(recv_g, MAIN, E, 1)
        eye_s = hot(iota((S, S), 0) == iota((S, S), 1))
        rest = jnp.zeros((S, QD), F32)
        for q in range(SPLIT):
            cols = slice(q * QD, (q + 1) * QD)
            send_b[:, cols] = dot_nt(eye_s, rbT[cols, 0:S]).astype(BF16)
            rest += dot_nt(pack_pick(q), rbT[cols, S:ROWS])
        send_b[:, D : D + QD] = rest.astype(BF16)
        terms = jnp.broadcast_to(gt[0:1, :], (128, ROWS)).astype(BF16)
        r = iota((S, R), 1)
        s_ = iota((S, R), 0)
        any_pick = hot((s_ // MAIN == r // REST) & (lax.rem(s_, REST) == lax.rem(r, REST)))
        term_main = dot_nt(eye_s, terms[:, 0:S])
        term_rest = dot_nt(any_pick, terms[:, S:ROWS])
        send_b[:, D + QD : D + QD + 128] = jnp.where(
            iota((S, 128), 1) < 64, term_main, term_rest
        ).astype(BF16)
        to_plane_far(send_b, recv_b, MAIN, 4, D + QD + 128)
        own_block(send_b, True, recv_b, me, MAIN)

    def spread_grad(v):
        average = jnp.mean(v, axis=0, keepdims=True)
        dev = jnp.mean((v - average) ** 2, axis=0, keepdims=True)
        return (2.0 * (v - average) - 2.0 * dev / average) / (E * average * average)

    def at_home():
        received(sr2, 8, NZ, 3)
        received(recv_b, MAIN, E, 4)
        total = sr2[0:8, :]
        for j in range(1, NZ):
            total += sr2[j * 8 : (j + 1) * 8, :]
        row = jnp.broadcast_to(total[0:1, :], (E, 128))
        imp = jnp.sum(jnp.where(lane_id == row_id, row, 0.0), axis=1, keepdims=True)
        ld = jnp.sum(jnp.where(lane_id == row_id + E, row, 0.0), axis=1, keepdims=True)
        imp_coef = TOTAL * spread_grad(imp)
        load_coef = TOTAL * spread_grad(ld)
        probs = probs_s[...]
        zscore = z_s[...]
        tile = recv_b[:, D + QD : D + QD + 128].astype(F32)
        weighted = sel[...].astype(F32) * tile[:, 0:1] + selr[0:S, :].astype(F32) * tile[:, 64:65]
        gather = hot(iota((E, S), 1) // MAIN == iota((E, S), 0))
        score = dot(gather, weighted.astype(BF16)) + imp_coef
        noisy_grad = probs * (score - jnp.sum(probs * score, axis=0, keepdims=True))
        z_grad = load_coef * inv_root_tau * jnp.exp(-0.5 * zscore * zscore)
        thresh = thr[...] == iota((E, T), 0)
        logit_grad = (
            noisy_grad
            + z_grad
            - jnp.where(thresh, jnp.sum(z_grad, axis=0, keepdims=True), 0.0)
        )
        low = logit_grad.astype(BF16)
        llT_s[...] = low
        weight_part = dot(low, patches[...])
        bias_col = jnp.sum(logit_grad, axis=1, keepdims=True)
        bias_row = jnp.sum(jnp.where(lane_id == row_id, bias_col, 0.0), axis=0, keepdims=True)
        bias_tile = jnp.broadcast_to(bias_row, (8, 128))
        tiles = D // 128
        for p in range(E):
            a, b = p // tiles, p % tiles
            ws1[p * 16 : p * 16 + 8, :] = weight_part[a * 8 : a * 8 + 8, b * 128 : b * 128 + 128]
            ws1[p * 16 + 8 : p * 16 + 16, :] = bias_tile
        to_plane(ws1, True, wr1, 16, 5)
        own_block(ws1, True, wr1, me, 16)

    def patches_out():
        low_rows = dot_nt(eye_t, llT_s[...]).astype(BF16)
        for q in range(SPLIT):
            cols = slice(q * QD, (q + 1) * QD)
            out = dot(selT[...], recv_b[:, cols])
            out += dot(selrT[pl.ds(q * T, T), :], recv_b[:, D : D + QD])
            out += dot(low_rows, rwT[:, cols])
            pg[:, cols] = out.astype(BF16)
        whole_outs[0].start()

    def reduce_plane():
        patches_out()
        received(wr1, 16, E, 5)
        total = wr1[0:16, :]
        for j in range(1, E):
            total += wr1[j * 16 : (j + 1) * 16, :]
        ws2[...] = total
        to_line(ws2, wr2, 16, 6)
        own_block(ws2, False, wr2, z, 16)

    def reduce_line():
        received(wr2, 16, NZ, 6)
        total = wr2[0:16, :]
        for j in range(1, NZ):
            total += wr2[j * 16 : (j + 1) * 16, :]
        rb[...] = total[8:16, :]
        whole_outs[1].start()
        ws3[...] = total[0:8, :]
        to_plane(ws3, False, wr3, 8, 7)
        own_block(ws3, False, wr3, me, 8)

    def spread_total():
        received(wr3, 8, E, 7)
        tiles = D // 128
        for p in range(E):
            a, b = p // tiles, p % tiles
            rgT[a * 8 : a * 8 + 8, b * 128 : b * 128 + 128] = wr3[p * 8 : p * 8 + 8, :]
        whole_outs[2].start()

    works = (rows_home, at_home, reduce_plane, reduce_line, spread_total)
    gaps = dict(zip((2, 4, 5, 6), works)) if NZ == 8 else {}
    product(0, 0)
    ring_first(0)
    chunk_b(at_offset(1), True)
    product(0, 1)
    ring_first(1)
    G[0:S, :] = recv_g[:, 0:D]
    half = NZ // 2
    for s in range(NZ - 1):
        if s > 0:
            ring_step(s)
        if s == 0:
            backs(2, half + 1)
        if s == 1 or NZ == 2:
            backs(half + 1, NZ + 1)
        product(s + 1, 0)
        product(s + 1, 1)
        if s == 1 or NZ == 2:
            stats_on()
        if s in gaps:
            gaps[s]()
    ring_end(0, NSUB - 1)
    for work in works[len(gaps):]:
        work()
    ring_end(NSUB - 1, NSUB)

    sent(recv_x, MAIN, E, 0)
    sent(sr1, 8, E, 2)
    sent(sr2, 8, NZ, 3)
    sent(recv_b, MAIN, E, 4)
    sent(wr1, 16, E, 5)
    sent(wr2, 16, NZ, 6)
    sent(wr3, 8, E, 7)
    sent(rgate, 1, E, 8)

    def drain(i, c):
        for k, way in enumerate(ways):
            wait_bytes(way[2].at[pl.ds(0, SUB)], ring_sem.at[2 * k, i])
        return c

    lax.fori_loop(0, (NZ - 1) * NSUB, drain, 0)

    for copy in whole_outs:
        copy.wait()

    def written(h, c):
        piece_out(0, h).wait()
        piece_out(1, h).wait()
        return c

    lax.fori_loop(0, NSUB, written, 0)


def finish(pg, wiT, wo, rgT, rb, pg_out, wi_out, wo_out, rgT_out, rb_out, a, b, bT, c, d, e, f, sem):
    def move(src, dst, i):
        return pltpu.make_async_copy(src, dst, sem.at[i])

    ins = [move(s, t, i) for i, (s, t) in enumerate(((wiT, b), (pg, a), (wo, c), (rgT, d), (rb, e)))]
    outs = [
        move(s, t, 5 + i)
        for i, (s, t) in enumerate(
            ((bT, wi_out), (a, pg_out), (c, wo_out), (d, rgT_out), (f, rb_out))
        )
    ]
    for copy in ins:
        copy.start()
    for i in (1, 2, 3):
        ins[i].wait()
        outs[i].start()
    ins[0].wait()
    bT[...] = b[...].T
    outs[0].start()
    ins[4].wait()
    f[...] = e[0:1, 0 : f.shape[1]]
    outs[4].start()
    for copy in outs:
        copy.wait()


def on_device(
    patches, router_weight, router_bias, noise, top_experts, threshold_expert, w_in, w_out, out_grad
):
    T, D = patches.shape
    E = router_weight.shape[1]
    NZ = lax.axis_size("dp")
    F = w_in.shape[2]
    FC = F // NZ
    S = E * MAIN
    ROWS = S + E * REST
    QD = D // SPLIT
    WX = D + QD
    WG = WX + 128
    VMEM = pltpu.VMEM
    far = pl.BlockSpec(memory_space=pltpu.HBM)
    pg, wiT, wo, rgT, rb = pl.pallas_call(
        functools.partial(kernel, E, NZ, float(T * E * NZ)),
        out_shape=(
            jax.ShapeDtypeStruct((T, D), BF16),
            jax.ShapeDtypeStruct((FC, D), BF16),
            jax.ShapeDtypeStruct((FC, D), BF16),
            jax.ShapeDtypeStruct((E, D), F32),
            jax.ShapeDtypeStruct((8, 128), F32),
        ),
        in_specs=[far] * 9,
        out_specs=(far,) * 5,
        scratch_shapes=[
            VMEM((T, D), BF16), VMEM((FC, D), BF16), VMEM((FC, D), BF16), VMEM((E, D), F32),
            VMEM((8, 128), F32), pltpu.SemaphoreType.DMA((3 + 2 * NSUB,)),
            VMEM((E, 1, 128), F32), VMEM((E, 1, 128), F32),
            VMEM((E, D), BF16), VMEM((1, E), F32), VMEM((E, T), F32),
            VMEM((2, T), jnp.int32), VMEM((1, T), jnp.int32),
            VMEM((T, D), BF16), VMEM((T, D), BF16),
            VMEM((D, F), BF16), VMEM((F, D), BF16), VMEM((F, D), BF16),
            VMEM((SPLIT * E * REST, S), BF16), VMEM((F, ROWS), F32), VMEM((2 * FC, D), F32),
            VMEM((S, T), BF16), VMEM((SPLIT * S, T), BF16),
            VMEM((T, S), BF16), VMEM((SPLIT * T, S), BF16),
            VMEM((S, WX), BF16), VMEM((S, WG), BF16), VMEM((S, WX), BF16), VMEM((S, WX), BF16),
            VMEM((S, WG), BF16),
            VMEM((ROWS, D), BF16), VMEM((ROWS, D), BF16), VMEM((ROWS, D), BF16),
            VMEM((F, ROWS), BF16), VMEM((F, ROWS), BF16),
            VMEM((8, ROWS), F32), VMEM((8, ROWS), F32),
            VMEM(((NZ - 1) * FC, D), BF16),
            VMEM(((NZ - 1) * FC, D), BF16),
            VMEM((E, T), F32), VMEM((E, T), F32), VMEM((E, T), BF16),
            VMEM((8, 128), F32), VMEM((E * 8, 128), F32),
            VMEM((8, 128), F32), VMEM((NZ * 8, 128), F32),
            VMEM((E * 16, 128), F32), VMEM((E * 16, 128), F32),
            VMEM((16, 128), F32), VMEM((NZ * 16, 128), F32),
            VMEM((8, 128), F32), VMEM((E * 8, 128), F32),
            pltpu.SemaphoreType.DMA((9,)),
            pltpu.SemaphoreType.DMA((18,)),
            pltpu.SemaphoreType.DMA((4, (NZ - 1) * NSUB)),
        ],
        compiler_params=pltpu.CompilerParams(
            collective_id=0, has_side_effects=True, vmem_limit_bytes=58 * 1024 * 1024
        ),
        name="moe_back",
    )(
        patches,
        router_weight.T,
        router_bias.reshape(1, E),
        noise.T,
        top_experts.T,
        threshold_expert.reshape(1, T),
        out_grad,
        w_in[0],
        w_out[0],
    )
    pg, wi, wo, rgT, rb = pl.pallas_call(
        finish,
        out_shape=(
            jax.ShapeDtypeStruct((T, D), BF16),
            jax.ShapeDtypeStruct((D, FC), BF16),
            jax.ShapeDtypeStruct((FC, D), BF16),
            jax.ShapeDtypeStruct((E, D), F32),
            jax.ShapeDtypeStruct((1, E), F32),
        ),
        in_specs=[far] * 5,
        out_specs=(far,) * 5,
        scratch_shapes=[
            VMEM((T, D), BF16), VMEM((FC, D), BF16), VMEM((D, FC), BF16), VMEM((FC, D), BF16),
            VMEM((E, D), F32), VMEM((8, 128), F32), VMEM((1, E), F32),
            pltpu.SemaphoreType.DMA((10,)),
        ],
        compiler_params=pltpu.CompilerParams(vmem_limit_bytes=62 * 1024 * 1024),
        name="moe_back_out",
    )(pg, wiT, wo, rgT, rb)
    return (pg, wi[None], wo[None], rgT.T, rb[0])


def solution(mesh):
    both = ("expert", "dp")
    in_specs = (
        P(both, None), P(), P(), P(both, None), P(both, None), P(both),
        P("expert", None, None), P("expert", None, None), P(both, None),
    )
    out_specs = (P(both, None), P("expert", None, "dp"), P("expert", "dp", None), P(), P())
    return jax.shard_map(
        on_device, mesh=mesh, in_specs=in_specs, out_specs=out_specs, check_vma=False
    )
```
